256 devices in a mesh: grp: 8 (over x, core), lat: 32 (over y, z).
Axes of the slice: x: 4, y: 4, z: 8, core: 2. Of those that a mesh axis runs over, the one named last changes fastest.
Arguments:
- grid_state: bfloat16 [32, 192, 384, 128], P('grp', 'lat'), may hold values from -6 to 6
- noise_field: bfloat16 [32, 192, 384, 128], P('grp', 'lat'), may hold values from -6 to 6
- legendre: bfloat16 [192, 128, 128], P('lat'), may hold values from -0.4375 to 0.4375
- diffusion: float32 [128], replicated, may hold values from 0.1 to 10
- input_weight: bfloat16 [128, 256], replicated, may hold values from -0.5 to 0.5
- noise_weight: bfloat16 [128, 256], replicated, may hold values from -0.5 to 0.5
- input_bias: float32 [256], replicated, may hold values from -4 to 4
- middle_weight: bfloat16 [256, 256], replicated, may hold values from -0.375 to 0.375
- output_weight: bfloat16 [256, 128], replicated, may hold values from -0.375 to 0.375
Outputs:
- new_state: bfloat16 [32, 192, 384, 128], P('grp', 'lat')
- ens_mean: float32 [192, 384, 128], P('lat')
- ens_var: float32 [192, 384, 128], P('lat')
The draws below stay inside these ranges and needn't reach their ends.
All inputs are finite; a program needn't handle non-finite values.
Results may differ from the reference program's by a relative error of at most 0.012.
Values may be sent and summed in bfloat16 or wider, within the bound.
A program may use at most 128 MiB of HBM per device.

```python
import math
import jax
import jax.numpy as jnp
from jax import lax

CHAN = 128
NLON = 384
NLAT = 192
WAVES = 128
NOISE = 128
HIDDEN_SIZE = 256
MEMBERS = 32


def levels(key, extent, shards, low, largest):
    loudness = 1.0
    for dim, blocks in shards:
        draws = jax.random.uniform(jax.random.fold_in(jax.random.fold_in(key, 6), dim), (blocks,), jnp.float32, low / len(shards), largest / len(shards))
        loudness = loudness * jnp.repeat(jnp.exp(draws), extent[dim] // blocks).reshape((-1,) + (1,) * (len(extent) - 1 - dim))
    return loudness


def gaussian(own_key, shape, deviation, most, pieces=(), held_as=jnp.bfloat16):
    result = jax.random.normal(own_key, shape, jnp.float32) * deviation
    if len(pieces) > 0:
        result = levels(own_key, shape, pieces, -0.22, 0.18) * result
    return jnp.clip(result, min=-most, max=most).astype(held_as)


def setup_inputs(seed: int = 0) -> dict:
    arg_keys = jax.random.split(jax.random.key(seed), 10)
    grid_state = gaussian(arg_keys[0], (MEMBERS, NLAT, NLON, CHAN), 1.0, 6.0, ((0, 8), (1, 32)))
    noise_field = gaussian(arg_keys[1], (MEMBERS, NLAT, NLON, NOISE), 1.0, 6.0, ((0, 8), (1, 32)))
    legendre = gaussian(arg_keys[2], (NLAT, WAVES, WAVES), NLAT ** -0.5, 0.4375, ((0, 32),))
    diffusion = jnp.clip(jnp.exp(jax.random.uniform(arg_keys[3], (CHAN,), jnp.float32, math.log(0.1), math.log(10.0))), 0.1, 10.0)
    input_weight = gaussian(arg_keys[4], (CHAN, HIDDEN_SIZE), CHAN ** -0.5, 0.5)
    noise_weight = gaussian(arg_keys[5], (NOISE, HIDDEN_SIZE), NOISE ** -0.5, 0.5)
    input_bias = gaussian(arg_keys[6], (HIDDEN_SIZE,), 1.0, 4.0, (), jnp.float32)
    middle_weight = gaussian(arg_keys[7], (HIDDEN_SIZE, HIDDEN_SIZE), HIDDEN_SIZE ** -0.5, 0.375)
    output_weight = gaussian(arg_keys[8], (HIDDEN_SIZE, CHAN), HIDDEN_SIZE ** -0.5, 0.375)
    return {"grid_state": grid_state, "noise_field": noise_field, "legendre": legendre, "diffusion": diffusion, "input_weight": input_weight, "noise_weight": noise_weight, "input_bias": input_bias, "middle_weight": middle_weight, "output_weight": output_weight}


def wave_table(lon_count, wave_count):
    lon_ids = jnp.arange(lon_count, dtype=jnp.int32)[:, None]
    wave_ids = jnp.arange(wave_count, dtype=jnp.int32)[None, :]
    phase = (lon_ids * wave_ids % lon_count).astype(jnp.float32) * (2.0 * math.pi / lon_count)
    factor = math.sqrt(2.0 / lon_count)
    joined = jnp.concatenate([jnp.cos(phase), -jnp.sin(phase)], axis=1) * factor
    return joined.astype(jnp.bfloat16)

def damping_filter(diffusion, wave_count):
    degree = jnp.arange(wave_count, dtype=jnp.int32).astype(jnp.float32)
    ratio = degree * (degree + 1.0) / float((wave_count - 1) * wave_count)
    return 1.0 / (1.0 + diffusion[None, :] * (ratio * ratio)[:, None])

def reference(grid_state, noise_field, legendre, diffusion, input_weight, noise_weight, input_bias, middle_weight, output_weight):
    transform = wave_table(NLON, WAVES).astype(jnp.float32)
    legendre_values = legendre.astype(jnp.float32)
    wave_ids = jnp.arange(WAVES, dtype=jnp.int32)
    triangle = (wave_ids[None, :] >= wave_ids[:, None]).astype(jnp.float32)
    damping = damping_filter(diffusion, WAVES)

    def advance(pair):
        member_state, member_noise = pair
        fourier = jnp.einsum('lxc,xk->lkc', member_state.astype(jnp.float32), transform).astype(jnp.bfloat16)
        fourier = fourier.reshape(NLAT, 2, WAVES, CHAN).astype(jnp.float32)
        spectrum = jnp.einsum('lmn,lrmc->rmnc', legendre_values, fourier) * triangle[None, :, :, None]
        filtered = (spectrum * damping[None, None, :, :]).astype(jnp.bfloat16)
        grid_fourier = jnp.einsum('lmn,rmnc->lrmc', legendre_values, filtered.astype(jnp.float32)).astype(jnp.bfloat16)
        grid_fourier = grid_fourier.reshape(NLAT, 2 * WAVES, CHAN).astype(jnp.float32)
        smoothed = jnp.einsum('lkc,xk->lxc', grid_fourier, transform)
        flat_fields = smoothed.reshape(-1, CHAN)
        smoothed_in = flat_fields.astype(jnp.bfloat16)
        pre_act = jnp.dot(smoothed_in, input_weight, preferred_element_type=jnp.float32)
        pre_act = pre_act + jnp.dot(member_noise.reshape(-1, NOISE), noise_weight, preferred_element_type=jnp.float32)
        hidden_one = jax.nn.silu(pre_act + input_bias).astype(jnp.bfloat16)
        hidden_two = jax.nn.silu(jnp.dot(hidden_one, middle_weight, preferred_element_type=jnp.float32)).astype(jnp.bfloat16)
        tendency = jnp.dot(hidden_two, output_weight, preferred_element_type=jnp.float32)
        return (flat_fields + tendency).astype(jnp.bfloat16).reshape(NLAT, NLON, CHAN)
    new_state = lax.map(advance, (grid_state, noise_field))
    member_values = new_state.astype(jnp.float32)
    ens_mean = lax.optimization_barrier(jnp.mean(member_values, axis=0))
    ens_var = lax.optimization_barrier(jnp.sum(jnp.square(member_values - ens_mean), axis=0)) / (MEMBERS - 1)
    return (new_state, ens_mean, ens_var)
```

```python
import functools
import math

import jax
import jax.numpy as jnp
from jax import lax
from jax.experimental import pallas as pl
from jax.experimental.pallas import tpu as pltpu
from jax.sharding import PartitionSpec as P

MESH = pl.DeviceIdType.MESH
F32 = jnp.float32
BF16 = jnp.bfloat16

NY, NZ = 4, 8
NT = NY * NZ
NG = 8
NB = 4
NL = 6
LP = 3
NX = 384
C = 128
MX = NX // NG


def dot(a, b):
    return jnp.dot(a, b, preferred_element_type=F32)


def silu(v):
    u = 0.5 * v
    return u + u * jnp.tanh(u)


def kernel(
    grid_h, noise_h, leg_h, tf, ti, damp, wcat, bias, wmid, wout,
    new_h, mean_h, var_h,
    gbuf, nbuf, obuf, leg, lsend, lrecv, send1, recv1, send2, recv2,
    work_a, work_b, pn, pt, dm, msend, mrecv, asend, arecv, mbuf, vbuf,
    in_sem, out_sem, l_ss, l_rs, s1_ss, s1_rs, s2_ss, s2_rs, m_ss, m_rs, a_ss, a_rs,
):
    me = lax.axis_index("lat")
    mg = lax.axis_index("grp")
    my, mz = me // NZ, lax.rem(me, NZ)

    def peer(k):
        j, dy = k // NY, lax.rem(k, NY)
        half = (j + 1) // 2
        dz = jnp.where(lax.rem(j, 2) == 1, NZ - half, half)
        return lax.rem(my + dy, NY) * NZ + lax.rem(mz + dz, NZ)

    def each_peer(body):
        def step(k, carry):
            body(peer(NT - k))
            return carry
        lax.fori_loop(1, NT, step, 0)

    def each_mate(body):
        def step(k, carry):
            body(lax.rem(mg + k, NG))
            return carry
        lax.fori_loop(1, NG, step, 0)

    barrier = pltpu.get_barrier_semaphore()
    each_peer(lambda t: pl.semaphore_signal(
        barrier, inc=1, device_id={"lat": t}, device_id_type=MESH))
    each_mate(lambda g: pl.semaphore_signal(
        barrier, inc=1, device_id={"grp": g}, device_id_type=MESH))

    leg_in = pltpu.make_async_copy(leg_h, leg, in_sem.at[0])
    leg_in.start()
    g_in = [pltpu.make_async_copy(grid_h.at[b], gbuf.at[b], in_sem.at[1 + b]) for b in range(NB)]
    for c in g_in:
        c.start()
    n_in = pltpu.make_async_copy(noise_h, nbuf, in_sem.at[5])
    n_in.start()

    leg_in.wait()
    work_a[pl.ds(0, NL * C), :] = leg[...].astype(F32).reshape(NL * C, C)

    def pack_leg(p, carry):
        lsend[p] = work_a[pl.ds(p, 4 * NL, stride=NT), :].astype(BF16)
        return carry
    lax.fori_loop(0, NT, pack_leg, 0)

    def forward(b):
        for q in range(LP):
            rhs = jnp.concatenate([gbuf[b, 2 * q], gbuf[b, 2 * q + 1]], axis=1)
            out = dot(tf[...], rhs)
            both = jnp.concatenate(
                [out[:, :C].reshape(NT, 8, C), out[:, C:].reshape(NT, 8, C)], axis=1)
            send1[b, :, pl.ds(16 * q, 16), :] = both.astype(BF16)

    def send_first(b):
        each_peer(lambda t: pltpu.make_async_remote_copy(
            src_ref=send1.at[b, t], dst_ref=recv1.at[b, me],
            send_sem=s1_ss.at[b], recv_sem=s1_rs.at[b],
            device_id={"lat": t}, device_id_type=MESH).start())
        recv1[b, me] = send1[b, me]

    def all_bytes(ref, sem):
        pltpu.make_async_copy(ref, ref, sem).wait()

    g_in[0].wait()
    forward(0)
    pl.semaphore_wait(barrier, NT - 1 + NG - 1)
    each_peer(lambda t: pltpu.make_async_remote_copy(
        src_ref=lsend.at[t], dst_ref=lrecv.at[me],
        send_sem=l_ss, recv_sem=l_rs, device_id={"lat": t}, device_id_type=MESH).start())
    lrecv[me] = lsend[me]
    send_first(0)
    for b in range(1, NB):
        g_in[b].wait()
        forward(b)
        send_first(b)

    all_bytes(lrecv.at[pl.ds(0, NT - 1)], l_rs)
    work_a[pl.ds(0, NT * 4 * NL), :] = lrecv[...].astype(F32).reshape(NT * 4 * NL, C)
    rows = lax.broadcasted_iota(jnp.int32, (C, C), 0)
    for i in range(4):
        basis = work_a[pl.ds(i, NT * NL, stride=4), :]
        pn[i] = basis.astype(BF16)
        pt[i] = basis.T.astype(BF16)
        keep = rows >= me + NT * i
        dm[i] = jnp.where(keep, damp[...], 0.0)

    def legendre(b, carry):
        all_bytes(recv1.at[b, pl.ds(0, NT - 1)], s1_rs.at[b])
        work_a[...] = recv1[b].astype(F32).reshape(NT * 48, C)
        for i in range(4):
            x0 = work_a[pl.ds(i, NT * NL, stride=8), :].astype(BF16)
            x1 = work_a[pl.ds(4 + i, NT * NL, stride=8), :].astype(BF16)
            spec = dot(pt[i], jnp.concatenate([x0, x1], axis=1))
            scale = dm[i]
            filt = (spec * jnp.concatenate([scale, scale], axis=1)).astype(BF16)
            back = dot(pn[i], filt)
            work_b[pl.ds(i, NT * NL, stride=8), :] = back[:, :C]
            work_b[pl.ds(4 + i, NT * NL, stride=8), :] = back[:, C:]
        vals = work_b[...].astype(BF16).reshape(NT, LP, 16, C)
        for q in range(LP):
            send2[q, :, b] = vals[:, q]
        return carry
    lax.fori_loop(0, NB, legendre, 0)

    for q in range(LP):
        each_peer(lambda t: pltpu.make_async_remote_copy(
            src_ref=send2.at[q, t], dst_ref=recv2.at[q, me],
            send_sem=s2_ss.at[q], recv_sem=s2_rs.at[q],
            device_id={"lat": t}, device_id_type=MESH).start())
        recv2[q, me] = send2[q, me]

    def combine(q):
        all_bytes(mrecv.at[q, pl.ds(0, NG - 1)], m_rs.at[q])
        total = mrecv[q, 0, 0].astype(F32)
        square = mrecv[q, 0, 1].astype(F32)
        for g in range(1, NG):
            total += mrecv[q, g, 0].astype(F32)
            square += mrecv[q, g, 1].astype(F32)
        mean = total * (1.0 / (NB * NG))
        for g in range(NG):
            off = mrecv[q, g, 0].astype(F32) * (1.0 / NB) - mean
            square += NB * (off * off)
        asend[q, 0] = mean.astype(BF16)
        asend[q, 1] = (square * (1.0 / (NB * NG - 1))).astype(BF16)
        each_mate(lambda g: pltpu.make_async_remote_copy(
            src_ref=asend.at[q], dst_ref=arecv.at[q, mg],
            send_sem=a_ss.at[q], recv_sem=a_rs.at[q],
            device_id={"grp": g}, device_id_type=MESH).start())
        arecv[q, mg] = asend[q]

    def finish(q):
        all_bytes(arecv.at[q, pl.ds(0, NG - 1)], a_rs.at[q])
        for g in range(NG):
            mbuf[pl.ds(2 * q, 2), pl.ds(MX * g, MX), :] = arecv[q, g, 0].astype(F32)
            vbuf[pl.ds(2 * q, 2), pl.ds(MX * g, MX), :] = arecv[q, g, 1].astype(F32)
        pltpu.make_async_copy(mbuf.at[pl.ds(2 * q, 2)], mean_h.at[pl.ds(2 * q, 2)], out_sem.at[LP + q]).start()
        pltpu.make_async_copy(vbuf.at[pl.ds(2 * q, 2)], var_h.at[pl.ds(2 * q, 2)], out_sem.at[2 * LP + q]).start()

    n_in.wait()
    for q in range(LP):
        all_bytes(recv2.at[q, pl.ds(0, NT - 1)], s2_rs.at[q])

        def column(b, carry):
            vals = recv2[q, :, b].astype(F32)
            f0 = vals[:, :8].reshape(NT * 8, C).astype(BF16)
            f1 = vals[:, 8:].reshape(NT * 8, C).astype(BF16)
            smooth = dot(ti[...], jnp.concatenate([f0, f1], axis=1))
            smooth = jnp.concatenate([smooth[:, :C], smooth[:, C:]], axis=0)
            noise = nbuf[b, pl.ds(2 * q, 2)].reshape(2 * NX, C)
            pre = dot(jnp.concatenate([smooth.astype(BF16), noise], axis=1), wcat[...])
            one = silu(pre + bias[...]).astype(BF16)
            two = silu(dot(one, wmid[...])).astype(BF16)
            new = (smooth + dot(two, wout[...])).astype(BF16)
            obuf[b, pl.ds(2 * q, 2)] = new.reshape(2, NX, C)
            return carry
        lax.fori_loop(0, NB, column, 0)

        def moments(g, carry):
            vals = [obuf[b, pl.ds(2 * q, 2), pl.ds(MX * g, MX), :].astype(F32) for b in range(NB)]
            total = (vals[0] + vals[1]) + (vals[2] + vals[3])
            mean = total * (1.0 / NB)
            offs = [v - mean for v in vals]
            square = (offs[0] * offs[0] + offs[1] * offs[1]) + (offs[2] * offs[2] + offs[3] * offs[3])
            msend[q, g, 0] = total.astype(BF16)
            msend[q, g, 1] = square.astype(BF16)
            return carry
        lax.fori_loop(0, NG, moments, 0)
        each_mate(lambda g: pltpu.make_async_remote_copy(
            src_ref=msend.at[q, g], dst_ref=mrecv.at[q, mg],
            send_sem=m_ss.at[q], recv_sem=m_rs.at[q],
            device_id={"grp": g}, device_id_type=MESH).start())
        mrecv[q, mg] = msend[q, mg]
        pltpu.make_async_copy(
            obuf.at[:, pl.ds(2 * q, 2)], new_h.at[:, pl.ds(2 * q, 2)], out_sem.at[q]).start()
        if q >= 1:
            combine(q - 1)
        if q >= 2:
            finish(q - 2)
    combine(LP - 1)
    finish(LP - 2)
    finish(LP - 1)

    all_bytes(lsend.at[pl.ds(0, NT - 1)], l_ss)
    for b in range(NB):
        all_bytes(send1.at[b, pl.ds(0, NT - 1)], s1_ss.at[b])
    for q in range(LP):
        all_bytes(send2.at[q, pl.ds(0, NT - 1)], s2_ss.at[q])
        all_bytes(msend.at[q, pl.ds(0, NG - 1)], m_ss.at[q])
        all_bytes(mrecv.at[q, pl.ds(0, NG - 1)], a_ss.at[q])
        pltpu.make_async_copy(
            obuf.at[:, pl.ds(2 * q, 2)], new_h.at[:, pl.ds(2 * q, 2)], out_sem.at[q]).wait()
        pltpu.make_async_copy(mbuf.at[pl.ds(2 * q, 2)], mean_h.at[pl.ds(2 * q, 2)], out_sem.at[LP + q]).wait()
        pltpu.make_async_copy(vbuf.at[pl.ds(2 * q, 2)], var_h.at[pl.ds(2 * q, 2)], out_sem.at[2 * LP + q]).wait()


def wave_values(lon, order):
    peer_id, rest = order // 8, lax.rem(order, 8)
    part, wave = rest // 4, peer_id + NT * lax.rem(rest, 4)
    phase = lax.rem(lon * wave, NX).astype(F32) * (2.0 * math.pi / NX)
    value = jnp.where(part == 0, jnp.cos(phase), -jnp.sin(phase))
    return (value * math.sqrt(2.0 / NX)).astype(BF16)


def damping_filter(diffusion, wave_count):
    degree = jnp.arange(wave_count, dtype=jnp.int32).astype(F32)
    ratio = degree * (degree + 1.0) / float((wave_count - 1) * wave_count)
    return 1.0 / (1.0 + diffusion[None, :] * (ratio * ratio)[:, None])


def per_device(grid_state, noise_field, legendre, diffusion, input_weight, noise_weight, input_bias,
               middle_weight, output_weight):
    iota = functools.partial(lax.broadcasted_iota, jnp.int32)
    tf = wave_values(iota((2 * C, NX), 1), iota((2 * C, NX), 0))
    ti = wave_values(iota((NX, 2 * C), 0), iota((NX, 2 * C), 1))
    damp = damping_filter(diffusion, C)
    wcat = jnp.concatenate([input_weight, noise_weight], axis=0)
    vm = pl.BlockSpec(memory_space=pltpu.VMEM)
    hbm = pl.BlockSpec(memory_space=pl.ANY)
    dma = pltpu.SemaphoreType.DMA
    V = pltpu.VMEM
    return pl.pallas_call(
        kernel,
        out_shape=(
            jax.ShapeDtypeStruct((NB, NL, NX, C), BF16),
            jax.ShapeDtypeStruct((NL, NX, C), F32),
            jax.ShapeDtypeStruct((NL, NX, C), F32),
        ),
        in_specs=[hbm] * 3 + [vm] * 7,
        out_specs=(hbm, hbm, hbm),
        scratch_shapes=[
            V((NB, NL, NX, C), BF16), V((NB, NL, NX, C), BF16), V((NB, NL, NX, C), BF16),
            V((NL, C, C), BF16), V((NT, 4 * NL, C), BF16), V((NT, 4 * NL, C), BF16),
            V((NB, NT, 48, C), BF16), V((NB, NT, 48, C), BF16),
            V((LP, NT, NB, 16, C), BF16), V((LP, NT, NB, 16, C), BF16),
            V((NT * 48, C), F32), V((NT * 48, C), F32),
            V((4, NT * NL, C), BF16), V((4, C, NT * NL), BF16), V((4, C, C), F32),
            V((LP, NG, 2, 2, MX, C), BF16), V((LP, NG, 2, 2, MX, C), BF16),
            V((LP, 2, 2, MX, C), BF16), V((LP, NG, 2, 2, MX, C), BF16),
            V((NL, NX, C), F32), V((NL, NX, C), F32),
            dma((6,)), dma((3 * LP,)), dma, dma, dma((NB,)), dma((NB,)), dma((LP,)), dma((LP,)),
            dma((LP,)), dma((LP,)), dma((LP,)), dma((LP,)),
        ],
        compiler_params=pltpu.CompilerParams(
            collective_id=0, has_side_effects=True, vmem_limit_bytes=60 * 1024 * 1024),
    )(grid_state, noise_field, legendre, tf, ti, damp, wcat, input_bias[None, :], middle_weight, output_weight)


def solution(mesh):
    in_specs = (P("grp", "lat", None, None), P("grp", "lat", None, None), P("lat", None, None)) + (P(),) * 6
    out_specs = (P("grp", "lat", None, None), P("lat", None, None), P("lat", None, None))
    return jax.shard_map(per_device, mesh=mesh, in_specs=in_specs, out_specs=out_specs, check_vma=False)
```

```python
import math

import jax
import jax.numpy as jnp
from jax import lax
from jax.experimental import pallas as pl
from jax.experimental.pallas import tpu as pltpu
from jax.sharding import PartitionSpec as P

MESH = pl.DeviceIdType.MESH
F32 = jnp.float32
BF16 = jnp.bfloat16

NY, NZ = 4, 8
NT = NY * NZ
NX4 = 4
NG = 8
NB = 4
NP = 2
NL = 6
NX = 384
C = 128
H = 256
MX = NX // NG
CHUNKS = ((0, 2), (2, 2), (4, 1), (5, 1))
NQ = len(CHUNKS)
MATES = ((2, 0), (2, 1), (1, 0), (3, 0), (1, 1), (3, 1), (0, 1))


def dot(a, b):
    return jnp.dot(a, b, preferred_element_type=F32)


def silu(v):
    u = 0.5 * v
    return u + u * jnp.tanh(u)


def angle(lon, wave):
    return lax.rem(lon * wave, NX).astype(F32) * (2.0 * math.pi / NX)


def all_bytes(ref, sem):
    pltpu.make_async_copy(ref, ref, sem).wait()


def kernel(
    grid_h, noise_h, leg_h, diff_h, win_h, wnoise_h, bias_h, wmid_h, wout_h,
    obuf, mbuf, vbuf,
    gbuf, nbuf, leg, diff, wcat, bias, wmid, wout, cosa, sina, tf, ti,
    lsend, lrecv, send1, recv1, send2, recv2, work_a, work_b, pn, pt, dm,
    msend, mrecv, asend, arecv,
    in_sem, l_ss, l_rs, k_ss, k_rs, s1_ss, s1_rs, s2_ss, s2_rs, m_ss, m_rs, a_ss, a_rs,
):
    lat, mg = lax.axis_index("lat"), lax.axis_index("grp")
    my, mz = lat // NZ, lax.rem(lat, NZ)
    me = mz * NY + my
    mx, mc = mg // 2, lax.rem(mg, 2)

    def each_peer(body):
        def step(n, carry):
            k = NT - n
            j, dy = k // NY, lax.rem(k, NY)
            half = (j + 1) // 2
            dz = jnp.where(lax.rem(j, 2) == 1, NZ - half, half)
            y, z = lax.rem(my + dy, NY), lax.rem(mz + dz, NZ)
            body(y * NZ + z, z * NY + y)
            return carry
        lax.fori_loop(1, NT, step, 0)

    def each_mate(body):
        for dx, dc in MATES:
            body(lax.rem(mx + dx, NX4) * 2 + lax.rem(mc + dc, 2))

    loads = [
        (grid_h.at[0], gbuf.at[0]), (grid_h.at[1], gbuf.at[1]), (grid_h.at[2], gbuf.at[2]), (grid_h.at[3], gbuf.at[3]),
        (leg_h, leg), (diff_h, diff), (win_h, wcat.at[pl.ds(0, C)]), (wnoise_h, wcat.at[pl.ds(C, C)]),
        (bias_h, bias), (wmid_h, wmid), (wout_h, wout), (noise_h, nbuf),
    ]
    loads = [pltpu.make_async_copy(s, d, in_sem.at[n]) for n, (s, d) in enumerate(loads)]
    loads[0].start()
    barrier = pltpu.get_barrier_semaphore()
    each_peer(lambda t, s: pl.semaphore_signal(
        barrier, inc=1, device_id={"lat": t}, device_id_type=MESH))
    each_mate(lambda g: pl.semaphore_signal(
        barrier, inc=1, device_id={"grp": g}, device_id_type=MESH))
    for c in loads[1:]:
        c.start()

    with jax.named_scope("tables"):
        iota = lambda shape, dim: lax.broadcasted_iota(jnp.int32, shape, dim)
        base = angle(iota((NT, NX), 1), iota((NT, NX), 0))
        cosa[...] = jnp.cos(base)
        sina[...] = jnp.sin(base)
        part = iota((8, NX), 0)
        step = angle(iota((8, NX), 1), NT * lax.rem(part, 4))
        scale = math.sqrt(2.0 / NX)
        cosb, sinb = scale * jnp.cos(step), scale * jnp.sin(step)
        real = part < 4
        u, v = jnp.where(real, cosb, -sinb), jnp.where(real, -sinb, -cosb)
        for j in range(NT // 2):
            pair = [cosa[pl.ds(p, 1), :] * u + sina[pl.ds(p, 1), :] * v for p in (2 * j, 2 * j + 1)]
            tf[pl.ds(16 * j, 16), :] = jnp.concatenate(pair, axis=0).astype(BF16)

    def forward(b):
        for q in range(NL // 2):
            rhs = jnp.concatenate([gbuf[b, 2 * q], gbuf[b, 2 * q + 1]], axis=1)
            out = dot(tf[...], rhs)
            both = jnp.concatenate(
                [out[:, :C].reshape(NT, 8, C), out[:, C:].reshape(NT, 8, C)], axis=1)
            send1[b, :, pl.ds(16 * q, 16), :] = both.astype(BF16)

    def send_first(b):
        each_peer(lambda t, s: pltpu.make_async_remote_copy(
            src_ref=send1.at[b, s], dst_ref=recv1.at[b, me],
            send_sem=s1_ss.at[b], recv_sem=s1_rs.at[b],
            device_id={"lat": t}, device_id_type=MESH).start())
        recv1[b, me] = send1[b, me]

    with jax.named_scope("w_g0"):
        loads[0].wait()
    with jax.named_scope("F0"):
        forward(0)
    loads[4].wait()

    source = mz == mg

    @pl.when(source)
    def _():
        work_a[pl.ds(0, NL * C), :] = leg[...].astype(F32).reshape(NL * C, C)

        def pack_leg(p, carry):
            lsend[p] = work_a[pl.ds(p, 4 * NL, stride=NT), :].astype(BF16)
            return carry
        lax.fori_loop(0, NT, pack_leg, 0)

    with jax.named_scope("barrier"):
        pl.semaphore_wait(barrier, NT - 1 + NG - 1)

    @pl.when(source)
    def _():
        each_peer(lambda t, s: pltpu.make_async_remote_copy(
            src_ref=lsend.at[s], dst_ref=lrecv.at[mz, my],
            send_sem=l_ss, recv_sem=l_rs, device_id={"lat": t}, device_id_type=MESH).start())
        lrecv[mz, my] = lsend[me]

    send_first(0)
    for b in range(1, NB):
        loads[b].wait()
        with jax.named_scope("F"):
            forward(b)
        with jax.named_scope("sF"):
            send_first(b)

    with jax.named_scope("w_leg"):
        @pl.when(source)
        def _():
            all_bytes(lrecv.at[mg, pl.ds(0, NY - 1)], l_rs)

        @pl.when(jnp.logical_not(source))
        def _():
            all_bytes(lrecv.at[mg], l_rs)

    each_mate(lambda g: pltpu.make_async_remote_copy(
        src_ref=lrecv.at[mg], dst_ref=lrecv.at[mg],
        send_sem=k_ss, recv_sem=k_rs, device_id={"grp": g}, device_id_type=MESH).start())
    with jax.named_scope("prep"):
        ti[...] = tf[...].astype(F32).T.astype(BF16)
        loads[5].wait()
        rows = iota((C, C), 0)
        degree = rows.astype(F32)
        ratio = degree * (degree + 1.0) / float((C - 1) * C)
        damp = 1.0 / (1.0 + diff[...] * (ratio * ratio))
        for i in range(4):
            dm[i] = jnp.where(rows >= me + NT * i, damp, 0.0)
    with jax.named_scope("w_k"):
        all_bytes(lrecv.at[pl.ds(0, NG - 1)], k_rs)
    with jax.named_scope("prepP"):
        work_a[pl.ds(0, NT * 4 * NL), :] = lrecv[...].astype(F32).reshape(NT * 4 * NL, C)
        for i in range(4):
            basis = work_a[pl.ds(i, NT * NL, stride=4), :]
            pn[i] = basis.astype(BF16)
            pt[i] = basis.T.astype(BF16)

    def send_second(l0, nl, pair, sem):
        def one(t, s):
            if pair is None:
                src, dst = send2.at[pl.ds(l0, nl), s], recv2.at[pl.ds(l0, nl), me]
            else:
                src, dst = send2.at[pl.ds(l0, nl), s, pair], recv2.at[pl.ds(l0, nl), me, pair]
            pltpu.make_async_remote_copy(
                src_ref=src, dst_ref=dst, send_sem=s2_ss.at[sem], recv_sem=s2_rs.at[sem],
                device_id={"lat": t}, device_id_type=MESH).start()
        each_peer(one)

    for pair in range(NP):
        def analyse(k, carry):
            b = NP * pair + k
            with jax.named_scope("w_a1"):
                all_bytes(recv1.at[b, pl.ds(0, NT - 1)], s1_rs.at[b])
            work_a[...] = recv1[b].astype(F32).reshape(NT * 48, C)
            for i in range(4):
                x0 = work_a[pl.ds(i, NT * NL, stride=8), :].astype(BF16)
                x1 = work_a[pl.ds(4 + i, NT * NL, stride=8), :].astype(BF16)
                spec = dot(pt[i], jnp.concatenate([x0, x1], axis=1))
                scale = dm[i]
                filt = (spec * jnp.concatenate([scale, scale], axis=1)).astype(BF16)
                back = dot(pn[i], filt)
                work_b[k, pl.ds(i, NT * NL, stride=8), :] = back[:, :C]
                work_b[k, pl.ds(4 + i, NT * NL, stride=8), :] = back[:, C:]
            return carry
        lax.fori_loop(0, 2, analyse, 0)
        vals = [work_b[k].reshape(NT, NL, 8, C) for k in range(2)]
        for l in range(NL):
            send2[l, :, pair] = jnp.concatenate([vals[0][:, l], vals[1][:, l]], axis=1).astype(BF16)
        with jax.named_scope("s2"):
            send_second(*CHUNKS[0], pair, pair)
    for q in range(1, NQ):
        send_second(*CHUNKS[q], None, q + 1)
    for l in range(NL):
        recv2[l, me] = send2[l, me]

    def combine(q):
        l0, nl = CHUNKS[q]
        with jax.named_scope("w_m"):
            all_bytes(mrecv.at[pl.ds(l0, nl), pl.ds(0, NG - 1)], m_rs.at[q])
        lats = pl.ds(l0, nl)
        total = mrecv[lats, 0, 0].astype(F32)
        square = mrecv[lats, 0, 1].astype(F32)
        for g in range(1, NG):
            total += mrecv[lats, g, 0].astype(F32)
            square += mrecv[lats, g, 1].astype(F32)
        mean = total * (1.0 / (NB * NG))
        for g in range(NG):
            off = mrecv[lats, g, 0].astype(F32) * (1.0 / NB) - mean
            square += NB * (off * off)
        asend[lats, 0] = mean.astype(BF16)
        asend[lats, 1] = (square * (1.0 / (NB * NG - 1))).astype(BF16)
        each_mate(lambda g: pltpu.make_async_remote_copy(
            src_ref=asend.at[lats], dst_ref=arecv.at[lats, mg],
            send_sem=a_ss.at[q], recv_sem=a_rs.at[q],
            device_id={"grp": g}, device_id_type=MESH).start())
        arecv[lats, mg] = asend[lats]

    def finish(q):
        l0, nl = CHUNKS[q]
        lats = pl.ds(l0, nl)
        with jax.named_scope("w_ag"):
            all_bytes(arecv.at[lats, pl.ds(0, NG - 1)], a_rs.at[q])
        for g in range(NG):
            mbuf[lats, pl.ds(MX * g, MX), :] = arecv[lats, g, 0].astype(F32)
            vbuf[lats, pl.ds(MX * g, MX), :] = arecv[lats, g, 1].astype(F32)

    for c in loads[6:]:
        c.wait()
    for q, (l0, nl) in enumerate(CHUNKS):
        with jax.named_scope("w_a2"):
            if q == 0:
                for pair in range(NP):
                    all_bytes(recv2.at[pl.ds(l0, nl), pl.ds(0, NT - 1), pair], s2_rs.at[pair])
            else:
                all_bytes(recv2.at[pl.ds(l0, nl), pl.ds(0, NT - 1)], s2_rs.at[q + 1])

        def column(n, carry):
            l, pair = l0 + n // NP, lax.rem(n, NP)
            vals = recv2[l, :, pair].astype(F32)
            f0 = vals[:, :8].reshape(NT * 8, C).astype(BF16)
            f1 = vals[:, 8:].reshape(NT * 8, C).astype(BF16)
            smooth = dot(ti[...], jnp.concatenate([f0, f1], axis=1))
            smooth = jnp.concatenate([smooth[:, :C], smooth[:, C:]], axis=0)
            noise = nbuf[pl.ds(2 * pair, 2), l].reshape(2 * NX, C)
            pre = dot(jnp.concatenate([smooth.astype(BF16), noise], axis=1), wcat[...])
            one = silu(pre + bias[...]).astype(BF16)
            two = silu(dot(one, wmid[...])).astype(BF16)
            new = (smooth + dot(two, wout[...])).astype(BF16)
            obuf[pl.ds(2 * pair, 2), l] = new.reshape(2, NX, C)
            return carry
        with jax.named_scope("G"):
            lax.fori_loop(0, nl * NP, column, 0)

        def moments(g, carry):
            lats = pl.ds(l0, nl)
            vals = [obuf[b, lats, pl.ds(MX * g, MX), :].astype(F32) for b in range(NB)]
            total = (vals[0] + vals[1]) + (vals[2] + vals[3])
            mean = total * (1.0 / NB)
            offs = [v - mean for v in vals]
            square = (offs[0] * offs[0] + offs[1] * offs[1]) + (offs[2] * offs[2] + offs[3] * offs[3])
            msend[lats, g, 0] = total.astype(BF16)
            msend[lats, g, 1] = square.astype(BF16)
            return carry
        with jax.named_scope("mom"):
            lax.fori_loop(0, NG, moments, 0)
        lats = pl.ds(l0, nl)
        each_mate(lambda g: pltpu.make_async_remote_copy(
            src_ref=msend.at[lats, g], dst_ref=mrecv.at[lats, mg],
            send_sem=m_ss.at[q], recv_sem=m_rs.at[q],
            device_id={"grp": g}, device_id_type=MESH).start())
        mrecv[lats, mg] = msend[lats, mg]
        if q >= 1:
            combine(q - 1)
        if q >= 2:
            finish(q - 2)
    combine(NQ - 1)
    finish(NQ - 2)
    finish(NQ - 1)

    with jax.named_scope("end"):
        @pl.when(source)
        def _():
            all_bytes(lsend.at[pl.ds(0, NT - 1)], l_ss)
        all_bytes(lrecv.at[pl.ds(0, NG - 1)], k_ss)
        for b in range(NB):
            all_bytes(send1.at[b, pl.ds(0, NT - 1)], s1_ss.at[b])
        for q, (l0, nl) in enumerate(CHUNKS):
            lats = pl.ds(l0, nl)
            if q == 0:
                for pair in range(NP):
                    all_bytes(send2.at[lats, pl.ds(0, NT - 1), pair], s2_ss.at[pair])
            else:
                all_bytes(send2.at[lats, pl.ds(0, NT - 1)], s2_ss.at[q + 1])
            all_bytes(msend.at[lats, pl.ds(0, NG - 1)], m_ss.at[q])
            all_bytes(arecv.at[lats, pl.ds(0, NG - 1)], a_ss.at[q])


def per_device(grid_state, noise_field, legendre, diffusion, input_weight, noise_weight, input_bias,
               middle_weight, output_weight):
    hbm = pl.BlockSpec(memory_space=pltpu.HBM)
    vm = pl.BlockSpec(memory_space=pltpu.VMEM)
    dma = pltpu.SemaphoreType.DMA
    V = pltpu.VMEM
    shapes = (((NB, NL, NX, C), BF16), ((NL, NX, C), F32), ((NL, NX, C), F32))
    return pl.pallas_call(
        kernel,
        out_shape=tuple(V(s, d) for s, d in shapes),
        in_specs=[hbm] * 9,
        out_specs=(vm, vm, vm),
        scratch_shapes=[
            V((NB, NL, NX, C), BF16), V((NB, NL, NX, C), BF16), V((NL, C, C), BF16), V((1, C), F32),
            V((H, H), BF16), V((1, H), F32), V((H, H), BF16), V((H, C), BF16),
            V((NT, NX), F32), V((NT, NX), F32), V((2 * C, NX), BF16), V((NX, 2 * C), BF16),
            V((NT, 4 * NL, C), BF16), V((NZ, NY, 4 * NL, C), BF16),
            V((NB, NT, 48, C), BF16), V((NB, NT, 48, C), BF16),
            V((NL, NT, NP, 16, C), BF16), V((NL, NT, NP, 16, C), BF16),
            V((NT * 48, C), F32), V((2, NT * 48, C), F32),
            V((4, NT * NL, C), BF16), V((4, C, NT * NL), BF16), V((4, C, C), F32),
            V((NL, NG, 2, MX, C), BF16), V((NL, NG, 2, MX, C), BF16),
            V((NL, 2, MX, C), BF16), V((NL, NG, 2, MX, C), BF16),
            dma((12,)), dma, dma, dma, dma, dma((NB,)), dma((NB,)), dma((NQ + 1,)), dma((NQ + 1,)),
            dma((NQ,)), dma((NQ,)), dma((NQ,)), dma((NQ,)),
        ],
        compiler_params=pltpu.CompilerParams(
            collective_id=0, has_side_effects=True, vmem_limit_bytes=48 * 1024 * 1024),
    )(*[pltpu.with_memory_space_constraint(a, pltpu.HBM) for a in (
        grid_state, noise_field, legendre, diffusion[None, :], input_weight, noise_weight, input_bias[None, :],
        middle_weight, output_weight)])

def solution(mesh):
    in_specs = (P("grp", "lat", None, None), P("grp", "lat", None, None), P("lat", None, None)) + (P(),) * 6
    out_specs = (P("grp", "lat", None, None), P("lat", None, None), P("lat", None, None))
    return jax.shard_map(per_device, mesh=mesh, in_specs=in_specs, out_specs=out_specs, check_vma=False)
```

```python
import math

import jax
import jax.numpy as jnp
from jax import lax
from jax.experimental import pallas as pl
from jax.experimental.pallas import tpu as pltpu
from jax.sharding import PartitionSpec as P

MESH = pl.DeviceIdType.MESH
F32 = jnp.float32
BF16 = jnp.bfloat16

NY, NZ = 4, 8
NT = NY * NZ
NX4 = 4
NG = 8
NB = 4
NP = 2
NL = 6
NX = 384
C = 128
H = 256
MX = NX // NG
CHUNKS = ((0, 2), (2, 2), (4, 1), (5, 1))
NQ = len(CHUNKS)
MATES = ((2, 0), (2, 1), (1, 0), (3, 0), (1, 1), (3, 1), (0, 1))


def dot(a, b):
    return jnp.dot(a, b, preferred_element_type=F32)


def silu(v):
    u = 0.5 * v
    return u + u * jnp.tanh(u)


def angle(lon, wave):
    return lax.rem(lon * wave, NX).astype(F32) * (2.0 * math.pi / NX)


def all_bytes(ref, sem):
    pltpu.make_async_copy(ref, ref, sem).wait()


def kernel(
    grid_h, noise_h, leg_h, diff_h, win_h, wnoise_h, bias_h, wmid_h, wout_h,
    obuf, mbuf, vbuf,
    gbuf, nbuf, leg, diff, wcat, bias, wmid, wout, cosa, sina, tf, ti,
    lsend, lrecv, send1, recv1, send2, recv2, work_a, work_b, pn, pt, dm,
    msend, mrecv, asend, arecv,
    in_sem, l_ss, l_rs, k_ss, k_rs, s1_ss, s1_rs, s2_ss, s2_rs, m_ss, m_rs, a_ss, a_rs,
):
    lat, mg = lax.axis_index("lat"), lax.axis_index("grp")
    my, mz = lat // NZ, lax.rem(lat, NZ)
    me = mz * NY + my
    mx, mc = mg // 2, lax.rem(mg, 2)

    def each_peer(body):
        def step(n, carry):
            k = NT - n
            j, dy = k // NY, lax.rem(k, NY)
            half = (j + 1) // 2
            dz = jnp.where(lax.rem(j, 2) == 1, NZ - half, half)
            y, z = lax.rem(my + dy, NY), lax.rem(mz + dz, NZ)
            body(y * NZ + z, z * NY + y)
            return carry
        lax.fori_loop(1, NT, step, 0)

    def each_mate(body):
        for dx, dc in MATES:
            body(lax.rem(mx + dx, NX4) * 2 + lax.rem(mc + dc, 2))

    loads = [
        (grid_h.at[0], gbuf.at[0]), (grid_h.at[1], gbuf.at[1]), (grid_h.at[2], gbuf.at[2]), (grid_h.at[3], gbuf.at[3]),
        (leg_h, leg), (diff_h, diff), (win_h, wcat.at[pl.ds(0, C)]), (wnoise_h, wcat.at[pl.ds(C, C)]),
        (bias_h, bias), (wmid_h, wmid), (wout_h, wout), (noise_h, nbuf),
    ]
    loads = [pltpu.make_async_copy(s, d, in_sem.at[n]) for n, (s, d) in enumerate(loads)]
    loads[0].start()
    barrier = pltpu.get_barrier_semaphore()
    each_peer(lambda t, s: pl.semaphore_signal(
        barrier, inc=1, device_id={"lat": t}, device_id_type=MESH))
    each_mate(lambda g: pl.semaphore_signal(
        barrier, inc=1, device_id={"grp": g}, device_id_type=MESH))
    for c in loads[1:]:
        c.start()

    with jax.named_scope("tables"):
        iota = lambda shape, dim: lax.broadcasted_iota(jnp.int32, shape, dim)
        base = angle(iota((NT, NX), 1), iota((NT, NX), 0))
        cosa[...] = jnp.cos(base)
        sina[...] = jnp.sin(base)
        part = iota((8, NX), 0)
        step = angle(iota((8, NX), 1), NT * lax.rem(part, 4))
        scale = math.sqrt(2.0 / NX)
        cosb, sinb = scale * jnp.cos(step), scale * jnp.sin(step)
        real = part < 4
        u, v = jnp.where(real, cosb, -sinb), jnp.where(real, -sinb, -cosb)
        for j in range(NT // 2):
            pair = [cosa[pl.ds(p, 1), :] * u + sina[pl.ds(p, 1), :] * v for p in (2 * j, 2 * j + 1)]
            tf[pl.ds(16 * j, 16), :] = jnp.concatenate(pair, axis=0).astype(BF16)

    def forward(b):
        for q in range(NL // 2):
            rhs = jnp.concatenate([gbuf[b, 2 * q], gbuf[b, 2 * q + 1]], axis=1)
            out = dot(tf[...], rhs)
            both = jnp.concatenate(
                [out[:, :C].reshape(NT, 8, C), out[:, C:].reshape(NT, 8, C)], axis=1)
            send1[b, :, pl.ds(16 * q, 16), :] = both.astype(BF16)

    def send_first(b):
        each_peer(lambda t, s: pltpu.make_async_remote_copy(
            src_ref=send1.at[b, s], dst_ref=recv1.at[b, me],
            send_sem=s1_ss.at[b], recv_sem=s1_rs.at[b],
            device_id={"lat": t}, device_id_type=MESH).start())
        recv1[b, me] = send1[b, me]

    with jax.named_scope("w_g0"):
        loads[0].wait()
    with jax.named_scope("F0"):
        forward(0)
    loads[4].wait()

    source = mz == mg

    @pl.when(source)
    def _():
        work_a[pl.ds(0, NL * C), :] = leg[...].astype(F32).reshape(NL * C, C)

        def pack_leg(p, carry):
            lsend[p] = work_a[pl.ds(p, 4 * NL, stride=NT), :].astype(BF16)
            return carry
        lax.fori_loop(0, NT, pack_leg, 0)

    with jax.named_scope("barrier"):
        pl.semaphore_wait(barrier, NT - 1 + NG - 1)

    @pl.when(source)
    def _():
        each_peer(lambda t, s: pltpu.make_async_remote_copy(
            src_ref=lsend.at[s], dst_ref=lrecv.at[mz, my],
            send_sem=l_ss, recv_sem=l_rs, device_id={"lat": t}, device_id_type=MESH).start())
        lrecv[mz, my] = lsend[me]

    send_first(0)
    for b in range(1, NB):
        loads[b].wait()
        with jax.named_scope("F"):
            forward(b)
        with jax.named_scope("sF"):
            send_first(b)

    with jax.named_scope("w_leg"):
        @pl.when(source)
        def _():
            all_bytes(lrecv.at[mg, pl.ds(0, NY - 1)], l_rs)

        @pl.when(jnp.logical_not(source))
        def _():
            all_bytes(lrecv.at[mg], l_rs)

    each_mate(lambda g: pltpu.make_async_remote_copy(
        src_ref=lrecv.at[mg], dst_ref=lrecv.at[mg],
        send_sem=k_ss, recv_sem=k_rs, device_id={"grp": g}, device_id_type=MESH).start())
    with jax.named_scope("prep"):
        ti[...] = tf[...].astype(F32).T.astype(BF16)
        loads[5].wait()
        rows = iota((C, C), 0)
        degree = rows.astype(F32)
        ratio = degree * (degree + 1.0) / float((C - 1) * C)
        damp = 1.0 / (1.0 + diff[...] * (ratio * ratio))
        for i in range(4):
            dm[i] = jnp.where(rows >= me + NT * i, damp, 0.0)
    with jax.named_scope("w_k"):
        all_bytes(lrecv.at[pl.ds(0, NG - 1)], k_rs)
    with jax.named_scope("prepP"):
        work_a[pl.ds(0, NT * 4 * NL), :] = lrecv[...].astype(F32).reshape(NT * 4 * NL, C)
        for i in range(4):
            basis = work_a[pl.ds(i, NT * NL, stride=4), :]
            pn[i] = basis.astype(BF16)
            pt[i] = basis.T.astype(BF16)

    def send_second(l0, nl, pair, sem):
        def one(t, s):
            if pair is None:
                src, dst = send2.at[pl.ds(l0, nl), s], recv2.at[pl.ds(l0, nl), me]
            else:
                src, dst = send2.at[pl.ds(l0, nl), s, pair], recv2.at[pl.ds(l0, nl), me, pair]
            pltpu.make_async_remote_copy(
                src_ref=src, dst_ref=dst, send_sem=s2_ss.at[sem], recv_sem=s2_rs.at[sem],
                device_id={"lat": t}, device_id_type=MESH).start()
        each_peer(one)

    for pair in range(NP):
        def analyse(k, carry):
            b = NP * pair + k
            with jax.named_scope("w_a1"):
                all_bytes(recv1.at[b, pl.ds(0, NT - 1)], s1_rs.at[b])
            work_a[...] = recv1[b].astype(F32).reshape(NT * 48, C)
            for i in range(4):
                x0 = work_a[pl.ds(i, NT * NL, stride=8), :].astype(BF16)
                x1 = work_a[pl.ds(4 + i, NT * NL, stride=8), :].astype(BF16)
                spec = dot(pt[i], jnp.concatenate([x0, x1], axis=1))
                scale = dm[i]
                filt = (spec * jnp.concatenate([scale, scale], axis=1)).astype(BF16)
                back = dot(pn[i], filt)
                work_b[k, pl.ds(i, NT * NL, stride=8), :] = back[:, :C]
                work_b[k, pl.ds(4 + i, NT * NL, stride=8), :] = back[:, C:]
            return carry
        lax.fori_loop(0, 2, analyse, 0)
        vals = [work_b[k].reshape(NT, NL, 8, C) for k in range(2)]
        for l in range(NL):
            send2[l, :, pair] = jnp.concatenate([vals[0][:, l], vals[1][:, l]], axis=1).astype(BF16)
        with jax.named_scope("s2"):
            send_second(*CHUNKS[0], pair, pair)
    for q in range(1, NQ):
        send_second(*CHUNKS[q], None, q + 1)
    for l in range(NL):
        recv2[l, me] = send2[l, me]

    def combine(q):
        l0, nl = CHUNKS[q]
        with jax.named_scope("w_m"):
            all_bytes(mrecv.at[pl.ds(l0, nl), pl.ds(0, NG - 1)], m_rs.at[q])
        lats = pl.ds(l0, nl)
        total = mrecv[lats, 0, 0].astype(F32)
        square = mrecv[lats, 0, 1].astype(F32)
        for g in range(1, NG):
            total += mrecv[lats, g, 0].astype(F32)
            square += mrecv[lats, g, 1].astype(F32)
        mean = total * (1.0 / (NB * NG))
        for g in range(NG):
            off = mrecv[lats, g, 0].astype(F32) * (1.0 / NB) - mean
            square += NB * (off * off)
        asend[lats, 0] = mean.astype(BF16)
        asend[lats, 1] = (square * (1.0 / (NB * NG - 1))).astype(BF16)
        each_mate(lambda g: pltpu.make_async_remote_copy(
            src_ref=asend.at[lats], dst_ref=arecv.at[lats, mg],
            send_sem=a_ss.at[q], recv_sem=a_rs.at[q],
            device_id={"grp": g}, device_id_type=MESH).start())
        arecv[lats, mg] = asend[lats]

    def finish(q):
        l0, nl = CHUNKS[q]
        lats = pl.ds(l0, nl)
        with jax.named_scope("w_ag"):
            all_bytes(arecv.at[lats, pl.ds(0, NG - 1)], a_rs.at[q])
        for g in range(NG):
            mbuf[lats, pl.ds(MX * g, MX), :] = arecv[lats, g, 0].astype(F32)
            vbuf[lats, pl.ds(MX * g, MX), :] = arecv[lats, g, 1].astype(F32)

    for c in loads[6:]:
        c.wait()
    for q, (l0, nl) in enumerate(CHUNKS):
        with jax.named_scope("w_a2"):
            if q == 0:
                for pair in range(NP):
                    all_bytes(recv2.at[pl.ds(l0, nl), pl.ds(0, NT - 1), pair], s2_rs.at[pair])
            else:
                all_bytes(recv2.at[pl.ds(l0, nl), pl.ds(0, NT - 1)], s2_rs.at[q + 1])

        def column(n, carry):
            l, pair = l0 + n // NP, lax.rem(n, NP)
            vals = recv2[l, :, pair].astype(F32)
            f0 = vals[:, :8].reshape(NT * 8, C).astype(BF16)
            f1 = vals[:, 8:].reshape(NT * 8, C).astype(BF16)
            smooth = dot(ti[...], jnp.concatenate([f0, f1], axis=1))
            smooth = jnp.concatenate([smooth[:, :C], smooth[:, C:]], axis=0)
            noise = nbuf[pl.ds(2 * pair, 2), l].reshape(2 * NX, C)
            pre = dot(jnp.concatenate([smooth.astype(BF16), noise], axis=1), wcat[...])
            one = silu(pre + bias[...]).astype(BF16)
            two = silu(dot(one, wmid[...])).astype(BF16)
            new = (smooth + dot(two, wout[...])).astype(BF16)
            obuf[pl.ds(2 * pair, 2), l] = new.reshape(2, NX, C)
            return carry
        with jax.named_scope("G"):
            lax.fori_loop(0, nl * NP, column, 0)

        def moments(g, carry):
            lats = pl.ds(l0, nl)
            vals = [obuf[b, lats, pl.ds(MX * g, MX), :].astype(F32) for b in range(NB)]
            total = (vals[0] + vals[1]) + (vals[2] + vals[3])
            mean = total * (1.0 / NB)
            offs = [v - mean for v in vals]
            square = (offs[0] * offs[0] + offs[1] * offs[1]) + (offs[2] * offs[2] + offs[3] * offs[3])
            msend[lats, g, 0] = total.astype(BF16)
            msend[lats, g, 1] = square.astype(BF16)
            return carry
        with jax.named_scope("mom"):
            lax.fori_loop(0, NG, moments, 0)
        lats = pl.ds(l0, nl)
        each_mate(lambda g: pltpu.make_async_remote_copy(
            src_ref=msend.at[lats, g], dst_ref=mrecv.at[lats, mg],
            send_sem=m_ss.at[q], recv_sem=m_rs.at[q],
            device_id={"grp": g}, device_id_type=MESH).start())
        mrecv[lats, mg] = msend[lats, mg]
        if q >= 1:
            combine(q - 1)
    combine(NQ - 1)
    for q in range(NQ):
        finish(q)

    with jax.named_scope("end"):
        @pl.when(source)
        def _():
            all_bytes(lsend.at[pl.ds(0, NT - 1)], l_ss)
        all_bytes(lrecv.at[pl.ds(0, NG - 1)], k_ss)
        for b in range(NB):
            all_bytes(send1.at[b, pl.ds(0, NT - 1)], s1_ss.at[b])
        for q, (l0, nl) in enumerate(CHUNKS):
            lats = pl.ds(l0, nl)
            if q == 0:
                for pair in range(NP):
                    all_bytes(send2.at[lats, pl.ds(0, NT - 1), pair], s2_ss.at[pair])
            else:
                all_bytes(send2.at[lats, pl.ds(0, NT - 1)], s2_ss.at[q + 1])
            all_bytes(msend.at[lats, pl.ds(0, NG - 1)], m_ss.at[q])
            all_bytes(arecv.at[lats, pl.ds(0, NG - 1)], a_ss.at[q])


def write_out(o, m, v, new_h, mean_h, var_h, sem):
    copies = [pltpu.make_async_copy(s, d, sem.at[n])
              for n, (s, d) in enumerate(((o, new_h), (m, mean_h), (v, var_h)))]
    for c in copies:
        c.start()
    for c in copies:
        c.wait()


def per_device(grid_state, noise_field, legendre, diffusion, input_weight, noise_weight, input_bias,
               middle_weight, output_weight):
    hbm = pl.BlockSpec(memory_space=pltpu.HBM)
    vm = pl.BlockSpec(memory_space=pltpu.VMEM)
    dma = pltpu.SemaphoreType.DMA
    V = pltpu.VMEM
    shapes = (((NB, NL, NX, C), BF16), ((NL, NX, C), F32), ((NL, NX, C), F32))
    held = pl.pallas_call(
        kernel,
        out_shape=tuple(V(s, d) for s, d in shapes),
        in_specs=[hbm] * 9,
        out_specs=(vm, vm, vm),
        scratch_shapes=[
            V((NB, NL, NX, C), BF16), V((NB, NL, NX, C), BF16), V((NL, C, C), BF16), V((1, C), F32),
            V((H, H), BF16), V((1, H), F32), V((H, H), BF16), V((H, C), BF16),
            V((NT, NX), F32), V((NT, NX), F32), V((2 * C, NX), BF16), V((NX, 2 * C), BF16),
            V((NT, 4 * NL, C), BF16), V((NZ, NY, 4 * NL, C), BF16),
            V((NB, NT, 48, C), BF16), V((NB, NT, 48, C), BF16),
            V((NL, NT, NP, 16, C), BF16), V((NL, NT, NP, 16, C), BF16),
            V((NT * 48, C), F32), V((2, NT * 48, C), F32),
            V((4, NT * NL, C), BF16), V((4, C, NT * NL), BF16), V((4, C, C), F32),
            V((NL, NG, 2, MX, C), BF16), V((NL, NG, 2, MX, C), BF16),
            V((NL, 2, MX, C), BF16), V((NL, NG, 2, MX, C), BF16),
            dma((12,)), dma, dma, dma, dma, dma((NB,)), dma((NB,)), dma((NQ + 1,)), dma((NQ + 1,)),
            dma((NQ,)), dma((NQ,)), dma((NQ,)), dma((NQ,)),
        ],
        compiler_params=pltpu.CompilerParams(
            collective_id=0, has_side_effects=True, vmem_limit_bytes=48 * 1024 * 1024),
    )(*[pltpu.with_memory_space_constraint(a, pltpu.HBM) for a in (
        grid_state, noise_field, legendre, diffusion[None, :], input_weight, noise_weight, input_bias[None, :],
        middle_weight, output_weight)])
    return pl.pallas_call(
        write_out,
        out_shape=tuple(jax.ShapeDtypeStruct(s, d) for s, d in shapes),
        in_specs=[vm] * 3,
        out_specs=(hbm,) * 3,
        scratch_shapes=[dma((3,))],
        compiler_params=pltpu.CompilerParams(vmem_limit_bytes=1024 * 1024),
    )(*[pltpu.with_memory_space_constraint(a, pltpu.VMEM) for a in held])

def solution(mesh):
    in_specs = (P("grp", "lat", None, None), P("grp", "lat", None, None), P("lat", None, None)) + (P(),) * 6
    out_specs = (P("grp", "lat", None, None), P("lat", None, None), P("lat", None, None))
    return jax.shard_map(per_device, mesh=mesh, in_specs=in_specs, out_specs=out_specs, check_vma=False)
```

```python
import math

import jax
import jax.numpy as jnp
from jax import lax
from jax.experimental import pallas as pl
from jax.experimental.pallas import tpu as pltpu
from jax.sharding import PartitionSpec as P

MESH = pl.DeviceIdType.MESH
F32 = jnp.float32
BF16 = jnp.bfloat16

NY, NZ = 4, 8
NT = NY * NZ
NX4 = 4
NG = 8
NB = 4
NP = 2
NL = 6
NX = 384
C = 128
H = 256
MX = NX // NG
CHUNKS = ((0, 2), (2, 2), (4, 1), (5, 1))
NQ = len(CHUNKS)
MATES = ((2, 0), (2, 1), (1, 0), (3, 0), (1, 1), (3, 1), (0, 1))
LINE = (2, 1, 3)


def dot(a, b):
    return jnp.dot(a, b, preferred_element_type=F32)


def silu(v):
    u = 0.5 * v
    return u + u * jnp.tanh(u)


def angle(lon, wave):
    return lax.rem(lon * wave, NX).astype(F32) * (2.0 * math.pi / NX)


def all_bytes(ref, sem):
    pltpu.make_async_copy(ref, ref, sem).wait()


def kernel(
    grid_h, noise_h, leg_h, diff_h, win_h, wnoise_h, bias_h, wmid_h, wout_h,
    obuf, mbuf, vbuf,
    gbuf, nbuf, leg, diff, wcat, bias, wmid, wout, cosa, sina, tf, ti,
    lsend, lrecv, send1, recv1, send2, recv2, work_a, work_b, pn, pt, dm,
    msend, hrecv, csend, mrecv, asend, arecv,
    in_sem, l_ss, l_rs, k_ss, k_rs, s1_ss, s1_rs, s2_ss, s2_rs, h_ss, h_rs, m_ss, m_rs, a_ss, a_rs,
):
    lat, mg = lax.axis_index("lat"), lax.axis_index("grp")
    my, mz = lat // NZ, lax.rem(lat, NZ)
    me = mz * NY + my
    mx, mc = mg // 2, lax.rem(mg, 2)

    def each_peer(body):
        def step(n, carry):
            k = NT - n
            j, dy = k // NY, lax.rem(k, NY)
            half = (j + 1) // 2
            dz = jnp.where(lax.rem(j, 2) == 1, NZ - half, half)
            y, z = lax.rem(my + dy, NY), lax.rem(mz + dz, NZ)
            body(y * NZ + z, z * NY + y)
            return carry
        lax.fori_loop(1, NT, step, 0)

    def each_mate(body):
        for dx, dc in MATES:
            body(lax.rem(mx + dx, NX4) * 2 + lax.rem(mc + dc, 2))

    loads = [
        (grid_h.at[0], gbuf.at[0]), (grid_h.at[1], gbuf.at[1]), (grid_h.at[2], gbuf.at[2]), (grid_h.at[3], gbuf.at[3]),
        (leg_h, leg), (diff_h, diff), (win_h, wcat.at[pl.ds(0, C)]), (wnoise_h, wcat.at[pl.ds(C, C)]),
        (bias_h, bias), (wmid_h, wmid), (wout_h, wout), (noise_h, nbuf),
    ]
    loads = [pltpu.make_async_copy(s, d, in_sem.at[n]) for n, (s, d) in enumerate(loads)]
    loads[0].start()
    barrier = pltpu.get_barrier_semaphore()
    each_peer(lambda t, s: pl.semaphore_signal(
        barrier, inc=1, device_id={"lat": t}, device_id_type=MESH))
    each_mate(lambda g: pl.semaphore_signal(
        barrier, inc=1, device_id={"grp": g}, device_id_type=MESH))
    for c in loads[1:]:
        c.start()

    with jax.named_scope("tables"):
        iota = lambda shape, dim: lax.broadcasted_iota(jnp.int32, shape, dim)
        base = angle(iota((NT, NX), 1), iota((NT, NX), 0))
        cosa[...] = jnp.cos(base)
        sina[...] = jnp.sin(base)
        part = iota((8, NX), 0)
        step = angle(iota((8, NX), 1), NT * lax.rem(part, 4))
        scale = math.sqrt(2.0 / NX)
        cosb, sinb = scale * jnp.cos(step), scale * jnp.sin(step)
        real = part < 4
        u, v = jnp.where(real, cosb, -sinb), jnp.where(real, -sinb, -cosb)
        for j in range(NT // 2):
            pair = [cosa[pl.ds(p, 1), :] * u + sina[pl.ds(p, 1), :] * v for p in (2 * j, 2 * j + 1)]
            tf[pl.ds(16 * j, 16), :] = jnp.concatenate(pair, axis=0).astype(BF16)

    def forward(b):
        for q in range(NL // 2):
            rhs = jnp.concatenate([gbuf[b, 2 * q], gbuf[b, 2 * q + 1]], axis=1)
            out = dot(tf[...], rhs)
            both = jnp.concatenate(
                [out[:, :C].reshape(NT, 8, C), out[:, C:].reshape(NT, 8, C)], axis=1)
            send1[b, :, pl.ds(16 * q, 16), :] = both.astype(BF16)

    def send_first(b):
        each_peer(lambda t, s: pltpu.make_async_remote_copy(
            src_ref=send1.at[b, s], dst_ref=recv1.at[b, me],
            send_sem=s1_ss.at[b], recv_sem=s1_rs.at[b],
            device_id={"lat": t}, device_id_type=MESH).start())
        recv1[b, me] = send1[b, me]

    with jax.named_scope("w_g0"):
        loads[0].wait()
    with jax.named_scope("F0"):
        forward(0)
    loads[4].wait()

    source = mz == mg

    @pl.when(source)
    def _():
        work_a[pl.ds(0, NL * C), :] = leg[...].astype(F32).reshape(NL * C, C)

        def pack_leg(p, carry):
            lsend[p] = work_a[pl.ds(p, 4 * NL, stride=NT), :].astype(BF16)
            return carry
        lax.fori_loop(0, NT, pack_leg, 0)

    with jax.named_scope("barrier"):
        pl.semaphore_wait(barrier, NT - 1 + NG - 1)

    @pl.when(source)
    def _():
        each_peer(lambda t, s: pltpu.make_async_remote_copy(
            src_ref=lsend.at[s], dst_ref=lrecv.at[mz, my],
            send_sem=l_ss, recv_sem=l_rs, device_id={"lat": t}, device_id_type=MESH).start())
        lrecv[mz, my] = lsend[me]

    send_first(0)
    for b in range(1, NB):
        loads[b].wait()
        with jax.named_scope("F"):
            forward(b)
        with jax.named_scope("sF"):
            send_first(b)

    with jax.named_scope("w_leg"):
        @pl.when(source)
        def _():
            all_bytes(lrecv.at[mg, pl.ds(0, NY - 1)], l_rs)

        @pl.when(jnp.logical_not(source))
        def _():
            all_bytes(lrecv.at[mg], l_rs)

    each_mate(lambda g: pltpu.make_async_remote_copy(
        src_ref=lrecv.at[mg], dst_ref=lrecv.at[mg],
        send_sem=k_ss, recv_sem=k_rs, device_id={"grp": g}, device_id_type=MESH).start())
    with jax.named_scope("prep"):
        ti[...] = tf[...].astype(F32).T.astype(BF16)
        loads[5].wait()
        rows = iota((C, C), 0)
        degree = rows.astype(F32)
        ratio = degree * (degree + 1.0) / float((C - 1) * C)
        damp = 1.0 / (1.0 + diff[...] * (ratio * ratio))
        for i in range(4):
            dm[i] = jnp.where(rows >= me + NT * i, damp, 0.0)
    with jax.named_scope("w_k"):
        all_bytes(lrecv.at[pl.ds(0, NG - 1)], k_rs)
    with jax.named_scope("prepP"):
        work_a[pl.ds(0, NT * 4 * NL), :] = lrecv[...].astype(F32).reshape(NT * 4 * NL, C)
        for i in range(4):
            basis = work_a[pl.ds(i, NT * NL, stride=4), :]
            pn[i] = basis.astype(BF16)
            pt[i] = basis.T.astype(BF16)

    def send_second(l0, nl, pair, sem):
        def one(t, s):
            if pair is None:
                src, dst = send2.at[pl.ds(l0, nl), s], recv2.at[pl.ds(l0, nl), me]
            else:
                src, dst = send2.at[pl.ds(l0, nl), s, pair], recv2.at[pl.ds(l0, nl), me, pair]
            pltpu.make_async_remote_copy(
                src_ref=src, dst_ref=dst, send_sem=s2_ss.at[sem], recv_sem=s2_rs.at[sem],
                device_id={"lat": t}, device_id_type=MESH).start()
        each_peer(one)

    for pair in range(NP):
        def analyse(k, carry):
            b = NP * pair + k
            with jax.named_scope("w_a1"):
                all_bytes(recv1.at[b, pl.ds(0, NT - 1)], s1_rs.at[b])
            work_a[...] = recv1[b].astype(F32).reshape(NT * 48, C)
            for i in range(4):
                x0 = work_a[pl.ds(i, NT * NL, stride=8), :].astype(BF16)
                x1 = work_a[pl.ds(4 + i, NT * NL, stride=8), :].astype(BF16)
                spec = dot(pt[i], jnp.concatenate([x0, x1], axis=1))
                scale = dm[i]
                filt = (spec * jnp.concatenate([scale, scale], axis=1)).astype(BF16)
                back = dot(pn[i], filt)
                work_b[k, pl.ds(i, NT * NL, stride=8), :] = back[:, :C]
                work_b[k, pl.ds(4 + i, NT * NL, stride=8), :] = back[:, C:]
            return carry
        lax.fori_loop(0, 2, analyse, 0)
        vals = [work_b[k].reshape(NT, NL, 8, C) for k in range(2)]
        for l in range(NL):
            send2[l, :, pair] = jnp.concatenate([vals[0][:, l], vals[1][:, l]], axis=1).astype(BF16)
        with jax.named_scope("s2"):
            send_second(*CHUNKS[0], pair, pair)
    for q in range(1, NQ):
        send_second(*CHUNKS[q], None, q + 1)
    for l in range(NL):
        recv2[l, me] = send2[l, me]

    def join(q):
        l0, nl = CHUNKS[q]
        lats = pl.ds(l0, nl)
        with jax.named_scope("w_h"):
            all_bytes(hrecv.at[lats], h_rs.at[q])

        def one(x, carry):
            mine, theirs = msend[lats, mc, x, 0].astype(F32), hrecv[lats, x, 0].astype(F32)
            off = mine - theirs
            square = msend[lats, mc, x, 1].astype(F32) + hrecv[lats, x, 1].astype(F32)
            csend[lats, x, 0] = (mine + theirs).astype(BF16)
            csend[lats, x, 1] = (square + off * off * (1.0 / (2 * NB))).astype(BF16)
            return carry
        lax.fori_loop(0, NX4, one, 0)
        for dx in LINE:
            x = lax.rem(mx + dx, NX4)
            pltpu.make_async_remote_copy(
                src_ref=csend.at[lats, x], dst_ref=mrecv.at[lats, mx],
                send_sem=m_ss.at[q], recv_sem=m_rs.at[q],
                device_id={"grp": x * 2 + mc}, device_id_type=MESH).start()
        mrecv[lats, mx] = csend[lats, mx]

    def combine(q):
        l0, nl = CHUNKS[q]
        with jax.named_scope("w_m"):
            all_bytes(mrecv.at[pl.ds(l0, nl), pl.ds(0, NX4 - 1)], m_rs.at[q])
        lats = pl.ds(l0, nl)
        total = mrecv[lats, 0, 0].astype(F32)
        square = mrecv[lats, 0, 1].astype(F32)
        for x in range(1, NX4):
            total += mrecv[lats, x, 0].astype(F32)
            square += mrecv[lats, x, 1].astype(F32)
        mean = total * (1.0 / (NB * NG))
        for x in range(NX4):
            off = mrecv[lats, x, 0].astype(F32) * (1.0 / (2 * NB)) - mean
            square += (2 * NB) * (off * off)
        asend[lats, 0] = mean.astype(BF16)
        asend[lats, 1] = (square * (1.0 / (NB * NG - 1))).astype(BF16)
        each_mate(lambda g: pltpu.make_async_remote_copy(
            src_ref=asend.at[lats], dst_ref=arecv.at[lats, mg],
            send_sem=a_ss.at[q], recv_sem=a_rs.at[q],
            device_id={"grp": g}, device_id_type=MESH).start())
        arecv[lats, mg] = asend[lats]

    def finish(q):
        l0, nl = CHUNKS[q]
        lats = pl.ds(l0, nl)
        with jax.named_scope("w_ag"):
            all_bytes(arecv.at[lats, pl.ds(0, NG - 1)], a_rs.at[q])
        for g in range(NG):
            mbuf[lats, pl.ds(MX * g, MX), :] = arecv[lats, g, 0].astype(F32)
            vbuf[lats, pl.ds(MX * g, MX), :] = arecv[lats, g, 1].astype(F32)

    for c in loads[6:]:
        c.wait()
    for q, (l0, nl) in enumerate(CHUNKS):
        with jax.named_scope("w_a2"):
            if q == 0:
                for pair in range(NP):
                    all_bytes(recv2.at[pl.ds(l0, nl), pl.ds(0, NT - 1), pair], s2_rs.at[pair])
            else:
                all_bytes(recv2.at[pl.ds(l0, nl), pl.ds(0, NT - 1)], s2_rs.at[q + 1])

        def column(n, carry):
            l, pair = l0 + n // NP, lax.rem(n, NP)
            vals = recv2[l, :, pair].astype(F32)
            f0 = vals[:, :8].reshape(NT * 8, C).astype(BF16)
            f1 = vals[:, 8:].reshape(NT * 8, C).astype(BF16)
            smooth = dot(ti[...], jnp.concatenate([f0, f1], axis=1))
            smooth = jnp.concatenate([smooth[:, :C], smooth[:, C:]], axis=0)
            noise = nbuf[pl.ds(2 * pair, 2), l].reshape(2 * NX, C)
            pre = dot(jnp.concatenate([smooth.astype(BF16), noise], axis=1), wcat[...])
            one = silu(pre + bias[...]).astype(BF16)
            two = silu(dot(one, wmid[...])).astype(BF16)
            new = (smooth + dot(two, wout[...])).astype(BF16)
            obuf[pl.ds(2 * pair, 2), l] = new.reshape(2, NX, C)
            return carry
        with jax.named_scope("G"):
            lax.fori_loop(0, nl * NP, column, 0)

        def moments(g, carry):
            lats = pl.ds(l0, nl)
            vals = [obuf[b, lats, pl.ds(MX * g, MX), :].astype(F32) for b in range(NB)]
            total = (vals[0] + vals[1]) + (vals[2] + vals[3])
            mean = total * (1.0 / NB)
            offs = [v - mean for v in vals]
            square = (offs[0] * offs[0] + offs[1] * offs[1]) + (offs[2] * offs[2] + offs[3] * offs[3])
            x, c = g // 2, lax.rem(g, 2)
            msend[lats, c, x, 0] = total.astype(BF16)
            msend[lats, c, x, 1] = square.astype(BF16)
            return carry
        with jax.named_scope("mom"):
            lax.fori_loop(0, NG, moments, 0)
        lats = pl.ds(l0, nl)
        pltpu.make_async_remote_copy(
            src_ref=msend.at[lats, 1 - mc], dst_ref=hrecv.at[lats],
            send_sem=h_ss.at[q], recv_sem=h_rs.at[q],
            device_id={"grp": mx * 2 + 1 - mc}, device_id_type=MESH).start()
        join(q)
        if q >= 1:
            combine(q - 1)
    combine(NQ - 1)
    for q in range(NQ):
        finish(q)

    with jax.named_scope("end"):
        @pl.when(source)
        def _():
            all_bytes(lsend.at[pl.ds(0, NT - 1)], l_ss)
        all_bytes(lrecv.at[pl.ds(0, NG - 1)], k_ss)
        for b in range(NB):
            all_bytes(send1.at[b, pl.ds(0, NT - 1)], s1_ss.at[b])
        for q, (l0, nl) in enumerate(CHUNKS):
            lats = pl.ds(l0, nl)
            if q == 0:
                for pair in range(NP):
                    all_bytes(send2.at[lats, pl.ds(0, NT - 1), pair], s2_ss.at[pair])
            else:
                all_bytes(send2.at[lats, pl.ds(0, NT - 1)], s2_ss.at[q + 1])
            all_bytes(hrecv.at[lats], h_ss.at[q])
            all_bytes(mrecv.at[lats, pl.ds(0, NX4 - 1)], m_ss.at[q])
            all_bytes(arecv.at[lats, pl.ds(0, NG - 1)], a_ss.at[q])


def write_out(o, m, v, new_h, mean_h, var_h, sem):
    copies = [pltpu.make_async_copy(s, d, sem.at[n])
              for n, (s, d) in enumerate(((o, new_h), (m, mean_h), (v, var_h)))]
    for c in copies:
        c.start()
    for c in copies:
        c.wait()


def per_device(grid_state, noise_field, legendre, diffusion, input_weight, noise_weight, input_bias,
               middle_weight, output_weight):
    hbm = pl.BlockSpec(memory_space=pltpu.HBM)
    vm = pl.BlockSpec(memory_space=pltpu.VMEM)
    dma = pltpu.SemaphoreType.DMA
    V = pltpu.VMEM
    shapes = (((NB, NL, NX, C), BF16), ((NL, NX, C), F32), ((NL, NX, C), F32))
    held = pl.pallas_call(
        kernel,
        out_shape=tuple(V(s, d) for s, d in shapes),
        in_specs=[hbm] * 9,
        out_specs=(vm, vm, vm),
        scratch_shapes=[
            V((NB, NL, NX, C), BF16), V((NB, NL, NX, C), BF16), V((NL, C, C), BF16), V((1, C), F32),
            V((H, H), BF16), V((1, H), F32), V((H, H), BF16), V((H, C), BF16),
            V((NT, NX), F32), V((NT, NX), F32), V((2 * C, NX), BF16), V((NX, 2 * C), BF16),
            V((NT, 4 * NL, C), BF16), V((NZ, NY, 4 * NL, C), BF16),
            V((NB, NT, 48, C), BF16), V((NB, NT, 48, C), BF16),
            V((NL, NT, NP, 16, C), BF16), V((NL, NT, NP, 16, C), BF16),
            V((NT * 48, C), F32), V((2, NT * 48, C), F32),
            V((4, NT * NL, C), BF16), V((4, C, NT * NL), BF16), V((4, C, C), F32),
            V((NL, 2, NX4, 2, MX, C), BF16), V((NL, NX4, 2, MX, C), BF16),
            V((NL, NX4, 2, MX, C), BF16), V((NL, NX4, 2, MX, C), BF16),
            V((NL, 2, MX, C), BF16), V((NL, NG, 2, MX, C), BF16),
            dma((12,)), dma, dma, dma, dma, dma((NB,)), dma((NB,)), dma((NQ + 1,)), dma((NQ + 1,)),
            dma((NQ,)), dma((NQ,)), dma((NQ,)), dma((NQ,)), dma((NQ,)), dma((NQ,)),
        ],
        compiler_params=pltpu.CompilerParams(
            collective_id=0, has_side_effects=True, vmem_limit_bytes=48 * 1024 * 1024),
    )(*[pltpu.with_memory_space_constraint(a, pltpu.HBM) for a in (
        grid_state, noise_field, legendre, diffusion[None, :], input_weight, noise_weight, input_bias[None, :],
        middle_weight, output_weight)])
    return pl.pallas_call(
        write_out,
        out_shape=tuple(jax.ShapeDtypeStruct(s, d) for s, d in shapes),
        in_specs=[vm] * 3,
        out_specs=(hbm,) * 3,
        scratch_shapes=[dma((3,))],
        compiler_params=pltpu.CompilerParams(vmem_limit_bytes=1024 * 1024),
    )(*[pltpu.with_memory_space_constraint(a, pltpu.VMEM) for a in held])

def solution(mesh):
    in_specs = (P("grp", "lat", None, None), P("grp", "lat", None, None), P("lat", None, None)) + (P(),) * 6
    out_specs = (P("grp", "lat", None, None), P("lat", None, None), P("lat", None, None))
    return jax.shard_map(per_device, mesh=mesh, in_specs=in_specs, out_specs=out_specs, check_vma=False)
```

```python
import functools
import math

import jax
import jax.numpy as jnp
from jax import lax
from jax.experimental import pallas as pl
from jax.experimental.pallas import tpu as pltpu
from jax.sharding import PartitionSpec as P

MESH = pl.DeviceIdType.MESH
F32 = jnp.float32
BF16 = jnp.bfloat16

NY, NZ = 4, 8
NT = NY * NZ
NX4 = 4
NG = 8
NB = 4
NP = 2
NL = 6
NX = 384
C = 128
H = 256
MX = NX // NG
CHUNKS = ((0, 2), (2, 2), (4, 1), (5, 1))
NQ = len(CHUNKS)
MATES = ((2, 0), (2, 1), (1, 0), (3, 0), (1, 1), (3, 1), (0, 1))
LINE = (2, 1, 3)
J = 6
NW = 8
SIZES = (32, 32, 24, 24, 16, 16, 8, 8)
OFFS = (0, 32, 64, 88, 112, 128, 144, 152)
NR = 160


def dot(a, b):
    return jnp.dot(a, b, preferred_element_type=F32)


def silu(v):
    u = 0.5 * v
    return u + u * jnp.tanh(u)


def angle(lon, wave):
    return lax.rem(lon * wave, NX).astype(F32) * (2.0 * math.pi / NX)


def all_bytes(ref, sem):
    pltpu.make_async_copy(ref, ref, sem).wait()


def band_column(col):
    wave = jnp.zeros_like(col)
    start = jnp.zeros_like(col)
    for w in range(1, NW):
        wave = wave + jnp.where(col >= OFFS[w], 1, 0)
        start = start + jnp.where(col >= OFFS[w], OFFS[w] - OFFS[w - 1], 0)
    return wave, col - start + 8 * (wave // 2)


def kernel(
    grid_h, noise_h, leg_h, diff_h, win_h, wnoise_h, bias_h, wmid_h, wout_h,
    obuf, mbuf, vbuf,
    gbuf, nbuf, leg, diff, wcat, bias, wmid, wout, cosa, sina, tf, ti,
    lsend, lrecv, qsend, qrecv, send1, recv1, send2a, recv2a, send2b, recv2b,
    t1send, t1recv, t3send, t3recv, dmat, dtm, scale3, rf, rp_send, rp_recv, rm_send, rm_recv, fall,
    zf, work_a, work_b, work_c, pn, pt, dm,
    msend, hrecv, csend, mrecv, asend, arecv,
    in_sem, l_ss, l_rs, k_ss, k_rs, q_ss, q_rs, t1_ss, t1_rs, t3_ss, t3_rs, rs_ss, rs_rs, ag_ss, ag_rs,
    s1_ss, s1_rs, s2_ss, s2_rs, h_ss, h_rs, m_ss, m_rs, a_ss, a_rs,
):
    lat, mg = lax.axis_index("lat"), lax.axis_index("grp")
    my, mz = lat // NZ, lax.rem(lat, NZ)
    me = mz * NY + my
    mx, mc = mg // 2, lax.rem(mg, 2)
    iota = lambda shape, dim: lax.broadcasted_iota(jnp.int32, shape, dim)

    def visit(j, dy, body):
        half = (j + 1) // 2
        dz = jnp.where(lax.rem(j, 2) == 1, NZ - half, half)
        y, z = lax.rem(my + dy, NY), lax.rem(mz + dz, NZ)
        body(y * NZ + z, z * NY + y)

    def each_peer(body):
        def step(n, carry):
            k = NT - n
            visit(k // NY, lax.rem(k, NY), body)
            return carry
        lax.fori_loop(1, NT, step, 0)

    def each_row(dy, body):
        def step(n, carry):
            visit(NZ - 1 - n, dy, body)
            return carry
        lax.fori_loop(0, NZ - (1 if dy == 0 else 0), step, 0)

    def each_mate(body):
        for dx, dc in MATES:
            body(lax.rem(mx + dx, NX4) * 2 + lax.rem(mc + dc, 2))

    def each_y(body):
        for dy in (2, 1, 3):
            y = lax.rem(my + dy, NY)
            body(y, y * NZ + mz)

    def around(d):
        return lax.rem(mz + d + NZ, NZ)

    def send(src, dst, ss, rs, lat_id):
        pltpu.make_async_remote_copy(
            src_ref=src, dst_ref=dst, send_sem=ss, recv_sem=rs,
            device_id={"lat": lat_id}, device_id_type=MESH).start()

    up, down = my * NZ + around(1), my * NZ + around(-1)

    loads = [
        (grid_h.at[0], gbuf.at[0]), (grid_h.at[1], gbuf.at[1]), (grid_h.at[2], gbuf.at[2]), (grid_h.at[3], gbuf.at[3]),
        (leg_h, leg), (diff_h, diff), (win_h, wcat.at[pl.ds(0, C)]), (wnoise_h, wcat.at[pl.ds(C, C)]),
        (bias_h, bias), (wmid_h, wmid), (wout_h, wout), (noise_h, nbuf),
    ]
    loads = [pltpu.make_async_copy(s, d, in_sem.at[n]) for n, (s, d) in enumerate(loads)]
    loads[0].start()
    loads[1].start()
    barrier = pltpu.get_barrier_semaphore()
    each_peer(lambda t, s: pl.semaphore_signal(
        barrier, inc=1, device_id={"lat": t}, device_id_type=MESH))
    each_mate(lambda g: pl.semaphore_signal(
        barrier, inc=1, device_id={"grp": g}, device_id_type=MESH))
    for c in loads[2:]:
        c.start()

    with jax.named_scope("tables"):
        base = angle(iota((NT, NX), 1), iota((NT, NX), 0))
        cosa[...] = jnp.cos(base)
        sina[...] = jnp.sin(base)
        part = iota((8, NX), 0)
        step = angle(iota((8, NX), 1), NT * lax.rem(part, 4))
        scale = math.sqrt(2.0 / NX)
        cosb, sinb = scale * jnp.cos(step), scale * jnp.sin(step)
        real = part < 4
        u, v = jnp.where(real, cosb, -sinb), jnp.where(real, -sinb, -cosb)
        for j in range(J):
            k = 4 * (j // 3) + j % 3
            tf[pl.ds(NT * j, NT), :] = (cosa[...] * u[k:k + 1] + sina[...] * v[k:k + 1]).astype(BF16)
        row = iota((NT, NX), 0)
        high = angle(iota((NT, NX), 1), NY * lax.rem(row, NW) + row // NW)
        cosq, sinq = jnp.cos(high), jnp.sin(high)
        for q in range(NY):
            co, si = cosq[NW * q:NW * (q + 1)], sinq[NW * q:NW * (q + 1)]
            pair = [co * u[k:k + 1] + si * v[k:k + 1] for k in (3, 7)]
            tf[pl.ds(J * NT + 16 * q, 16), :] = jnp.concatenate(pair, axis=0).astype(BF16)

    def forward(b):
        loads[b].wait()
        for n in range(NL // 2):
            rhs = jnp.concatenate([gbuf[b, 2 * n], gbuf[b, 2 * n + 1]], axis=1)
            out = dot(tf[...], rhs)
            high = []
            for k in range(2):
                lanes = out[:, k * C:(k + 1) * C]
                for j in range(J):
                    zf[pl.ds((2 * n + k) * 2 * J + (b % 2) * J + j, NT, stride=NL * 2 * J), :] = (
                        lanes[NT * j:NT * (j + 1)])
                high.append(lanes[J * NT:].reshape(NY, 2, NW, C))
            high = jnp.concatenate(high, axis=2).astype(BF16)
            for r in range(2):
                t1send[:, r * NB + b, pl.ds(16 * n, 16), :] = high[:, r]

    def pack(pair):
        send1[pair] = zf[...].astype(BF16).reshape(NT, NL * 2 * J, C)
        recv1[pair, me] = send1[pair, me]

    def send_first(pair, dy):
        each_row(dy, lambda t, s: send(
            send1.at[pair, s], recv1.at[pair, me], s1_ss.at[pair], s1_rs.at[pair], t))

    with jax.named_scope("F01"):
        forward(0)
        forward(1)
        pack(0)
    loads[4].wait()
    source = mz == mg
    with jax.named_scope("basis"):
        work_a[pl.ds(0, NL * C), :] = leg[...].astype(F32).reshape(NL * C, C)
        for q in range(NY):
            band = [work_a[pl.ds(C * l + 3 * NT + q, NW, stride=NY), :] for l in range(NL)]
            qsend[q] = jnp.concatenate(band, axis=0).astype(BF16)

        @pl.when(source)
        def _():
            def pack_leg(p, carry):
                lsend[p] = work_a[pl.ds(p, 4 * NL, stride=NT), :].astype(BF16)
                return carry
            lax.fori_loop(0, NT, pack_leg, 0)

    with jax.named_scope("barrier"):
        pl.semaphore_wait(barrier, NT - 1 + NG - 1)

    @pl.when(source)
    def _():
        each_peer(lambda t, s: send(lsend.at[s], lrecv.at[mz, my], l_ss, l_rs, t))
        lrecv[mz, my] = lsend[me]
    send_first(0, 1)
    each_y(lambda y, t: send(qsend.at[y], qrecv.at[my], q_ss, q_rs, t))
    qrecv[my] = qsend[my]
    send_first(0, 2)
    with jax.named_scope("F23"):
        forward(2)
        forward(3)
    each_y(lambda y, t: send(t1send.at[y], t1recv.at[my], t1_ss, t1_rs, t))
    t1recv[my] = t1send[my]
    with jax.named_scope("prep"):
        pack(1)
        loads[5].wait()
        rows = iota((C, C), 0)

        def damp_at(degree):
            ratio = degree.astype(F32) * (degree.astype(F32) + 1.0) / float((C - 1) * C)
            return 1.0 / (1.0 + diff[...] * (ratio * ratio))
        damp = damp_at(rows)
        for i in range(3):
            dm[i] = jnp.where(rows >= me + NT * i, damp, 0.0)
        wave, degree = band_column(iota((NR, C), 0))
        scale3[...] = jnp.where(degree >= NY * wave + my, damp_at(degree + 3 * NT), 0.0)
    with jax.named_scope("w_q"):
        all_bytes(qrecv.at[pl.ds(0, NY - 1)], q_rs)
    with jax.named_scope("dmat"):
        col = iota((C, 2 * C), 1)
        _, degree = band_column(col)
        pick = jnp.where((col < NR) & (iota((C, 2 * C), 0) == degree + 3 * NT), 1.0, 0.0).astype(BF16)
        spread = dot(qrecv[...].reshape(NY * NL * NW, C), pick)
        wave, _ = band_column(iota((NY * NL * NW, 2 * C), 1))
        spread = jnp.where(lax.rem(iota((NY * NL * NW, 2 * C), 0), NW) == wave, spread, 0.0)
        dtm[...] = spread[:, :NR].astype(BF16)
        dmat[...] = spread.T[:NR].astype(BF16)
    with jax.named_scope("w_t1"):
        all_bytes(t1recv.at[pl.ds(0, NY - 1)], t1_rs)
    with jax.named_scope("R"):
        for k in range(0, 8, 2):
            both = [t1recv[:, k + e].reshape(NY * NL * NW, C) for e in range(2)]
            out = dot(dmat[...], jnp.concatenate(both, axis=1))
            rf[k] = out[:, :C]
            rf[k + 1] = out[:, C:]

    def reduce_send(k):
        part = rf[around(4 - k)]
        if k > 0:
            part += rp_recv[k - 1].astype(F32)
        rp_send[k] = part.astype(BF16)
        if k < 3:
            part = rf[around(k - 3)]
            if k > 0:
                part += rm_recv[k - 1].astype(F32)
            rm_send[k] = part.astype(BF16)
        send(rp_send.at[k], rp_recv.at[k], rs_ss.at[0, k], rs_rs.at[0, k], up)
        if k < 3:
            send(rm_send.at[k], rm_recv.at[k], rs_ss.at[1, k], rs_rs.at[1, k], down)

    def reduce_wait(k):
        with jax.named_scope("w_rs"):
            all_bytes(rp_recv.at[k], rs_rs.at[0, k])
            if k < 3:
                all_bytes(rm_recv.at[k], rs_rs.at[1, k])

    def gather_send(k):
        a, b = around(-k), around(k)
        send(fall.at[a], fall.at[a], ag_ss.at[0, k], ag_rs.at[0, k], up)
        if k < 3:
            send(fall.at[b], fall.at[b], ag_ss.at[1, k], ag_rs.at[1, k], down)

    def gather_wait(k):
        with jax.named_scope("w_ring"):
            all_bytes(fall.at[0], ag_rs.at[0, k])
            if k < 3:
                all_bytes(fall.at[0], ag_rs.at[1, k])

    reduce_send(0)
    send_first(0, 3)
    with jax.named_scope("w_leg"):
        @pl.when(source)
        def _():
            all_bytes(lrecv.at[mg, pl.ds(0, NY - 1)], l_rs)

        @pl.when(jnp.logical_not(source))
        def _():
            all_bytes(lrecv.at[mg], l_rs)
    each_mate(lambda g: pltpu.make_async_remote_copy(
        src_ref=lrecv.at[mg], dst_ref=lrecv.at[mg],
        send_sem=k_ss, recv_sem=k_rs, device_id={"grp": g}, device_id_type=MESH).start())
    reduce_wait(0)
    reduce_send(1)
    send_first(0, 0)
    with jax.named_scope("prep2"):
        ti[...] = tf[...].astype(F32).T.astype(BF16)
    reduce_wait(1)
    reduce_send(2)
    send_first(1, 1)
    with jax.named_scope("w_k"):
        all_bytes(lrecv.at[pl.ds(0, NG - 1)], k_rs)
    with jax.named_scope("prepP"):
        work_a[pl.ds(0, NT * 4 * NL), :] = lrecv[...].astype(F32).reshape(NT * 4 * NL, C)
        for i in range(3):
            basis = jnp.concatenate(
                [work_a[pl.ds(4 * l + i, NT, stride=4 * NL), :] for l in range(NL)], axis=0)
            pn[i] = basis.astype(BF16)
            pt[i] = basis.T.astype(BF16)
    reduce_wait(2)
    reduce_send(3)
    send_first(1, 2)
    reduce_wait(3)
    total = rf[mz] + rp_recv[3].astype(F32) + rm_recv[2].astype(F32)
    fall[mz] = (total * scale3[...]).astype(BF16)
    gather_send(0)
    send_first(1, 3)
    gather_wait(0)
    gather_send(1)
    send_first(1, 0)

    def analyse(pair):
        with jax.named_scope("w_a1"):
            all_bytes(recv1.at[pair, pl.ds(0, NT - 1)], s1_rs.at[pair])

        def member(k, carry):
            for i in range(3):
                halves = [jnp.concatenate(
                    [work_a[pl.ds(2 * J * l + J * k + 3 * r + i, NT, stride=NL * 2 * J), :] for l in range(NL)],
                    axis=0).astype(BF16) for r in range(2)]
                spec = dot(pt[i], jnp.concatenate(halves, axis=1))
                scale = dm[i]
                filt = (spec * jnp.concatenate([scale, scale], axis=1)).astype(BF16)
                back = dot(pn[i], filt)
                for r in range(2):
                    j = 3 * r + i
                    for l in range(NL):
                        rows = back[NT * l:NT * (l + 1), r * C:(r + 1) * C]
                        if l < 2:
                            work_c[pl.ds(2 * J * l + J * k + j, NT, stride=4 * J), :] = rows
                        else:
                            work_b[l - 2, pl.ds(2 * J * pair + J * k + j, NT, stride=4 * J), :] = rows
            return carry
        with jax.named_scope("S"):
            work_a[...] = recv1[pair].astype(F32).reshape(NT * NL * 2 * J, C)
            lax.fori_loop(0, 2, member, 0)
            send2a[pair] = work_c[...].astype(BF16).reshape(NT, 4 * J, C)
            if pair == 1:
                for l in range(NL - 2):
                    send2b[l] = work_b[l].astype(BF16).reshape(NT, 4 * J, C)
        each_peer(lambda t, s: send(send2a.at[pair, s], recv2a.at[pair, me], s2_ss.at[pair], s2_rs.at[pair], t))
        recv2a[pair, me] = send2a[pair, me]

    gather_wait(1)
    gather_send(2)
    analyse(0)
    gather_wait(2)
    gather_send(3)
    analyse(1)
    for q in range(1, NQ):
        l0, nl = CHUNKS[q]
        lats = pl.ds(l0 - 2, nl)
        each_peer(lambda t, s: send(
            send2b.at[lats, s], recv2b.at[lats, me], s2_ss.at[q + 1], s2_rs.at[q + 1], t))
    for l in range(NL - 2):
        recv2b[l, me] = send2b[l, me]
    gather_wait(3)
    with jax.named_scope("synth"):
        for k in range(0, 8, 2):
            out = dot(dtm[...], jnp.concatenate([fall[k], fall[k + 1]], axis=1)).astype(BF16)
            t3send[:, k] = out[:, :C].reshape(NY, NL * NW, C)
            t3send[:, k + 1] = out[:, C:].reshape(NY, NL * NW, C)
    each_y(lambda y, t: send(t3send.at[y], t3recv.at[my], t3_ss, t3_rs, t))
    t3recv[my] = t3send[my]

    def join(q):
        l0, nl = CHUNKS[q]
        lats = pl.ds(l0, nl)
        with jax.named_scope("w_h"):
            all_bytes(hrecv.at[lats], h_rs.at[q])

        def one(x, carry):
            mine, theirs = msend[lats, mc, x, 0].astype(F32), hrecv[lats, x, 0].astype(F32)
            off = mine - theirs
            square = msend[lats, mc, x, 1].astype(F32) + hrecv[lats, x, 1].astype(F32)
            csend[lats, x, 0] = (mine + theirs).astype(BF16)
            csend[lats, x, 1] = (square + off * off * (1.0 / (2 * NB))).astype(BF16)
            return carry
        lax.fori_loop(0, NX4, one, 0)
        for dx in LINE:
            x = lax.rem(mx + dx, NX4)
            pltpu.make_async_remote_copy(
                src_ref=csend.at[lats, x], dst_ref=mrecv.at[lats, mx],
                send_sem=m_ss.at[q], recv_sem=m_rs.at[q],
                device_id={"grp": x * 2 + mc}, device_id_type=MESH).start()
        mrecv[lats, mx] = csend[lats, mx]

    def combine(q):
        l0, nl = CHUNKS[q]
        with jax.named_scope("w_m"):
            all_bytes(mrecv.at[pl.ds(l0, nl), pl.ds(0, NX4 - 1)], m_rs.at[q])
        lats = pl.ds(l0, nl)
        total = mrecv[lats, 0, 0].astype(F32)
        square = mrecv[lats, 0, 1].astype(F32)
        for x in range(1, NX4):
            total += mrecv[lats, x, 0].astype(F32)
            square += mrecv[lats, x, 1].astype(F32)
        mean = total * (1.0 / (NB * NG))
        for x in range(NX4):
            off = mrecv[lats, x, 0].astype(F32) * (1.0 / (2 * NB)) - mean
            square += (2 * NB) * (off * off)
        asend[lats, 0] = mean.astype(BF16)
        asend[lats, 1] = (square * (1.0 / (NB * NG - 1))).astype(BF16)
        each_mate(lambda g: pltpu.make_async_remote_copy(
            src_ref=asend.at[lats], dst_ref=arecv.at[lats, mg],
            send_sem=a_ss.at[q], recv_sem=a_rs.at[q],
            device_id={"grp": g}, device_id_type=MESH).start())
        arecv[lats, mg] = asend[lats]

    def finish(q):
        l0, nl = CHUNKS[q]
        lats = pl.ds(l0, nl)
        with jax.named_scope("w_ag"):
            all_bytes(arecv.at[lats, pl.ds(0, NG - 1)], a_rs.at[q])
        for g in range(NG):
            mbuf[lats, pl.ds(MX * g, MX), :] = arecv[lats, g, 0].astype(F32)
            vbuf[lats, pl.ds(MX * g, MX), :] = arecv[lats, g, 1].astype(F32)

    for c in loads[6:]:
        c.wait()
    with jax.named_scope("w_t3"):
        all_bytes(t3recv.at[pl.ds(0, NY - 1)], t3_rs)
    for q, (l0, nl) in enumerate(CHUNKS):
        with jax.named_scope("w_a2"):
            if q == 0:
                for pair in range(2):
                    all_bytes(recv2a.at[pair, pl.ds(0, NT - 1)], s2_rs.at[pair])
            else:
                all_bytes(recv2b.at[pl.ds(l0 - 2, nl), pl.ds(0, NT - 1)], s2_rs.at[q + 1])

        def column(l, pair, carry):
            if l < 2:
                work_c[...] = recv2a[pair].astype(F32).reshape(NT * 4 * J, C)
                first = 2 * J * l
            else:
                work_c[...] = recv2b[l - 2].astype(F32).reshape(NT * 4 * J, C)
                first = 2 * J * pair
            sides = []
            for k in range(2):
                rows = [work_c[pl.ds(first + J * k + j, NT, stride=4 * J), :] for j in range(J)]
                for y in range(NY):
                    for r in range(2):
                        two = t3recv[y, r * NB + 2 * pair + k, pl.ds(16 * (l // 2), 16), :].astype(F32)
                        rows.append(two[8 * (l % 2):8 * (l % 2) + 8])
                sides.append(jnp.concatenate(rows, axis=0).astype(BF16))
            smooth = dot(ti[...], jnp.concatenate(sides, axis=1))
            smooth = jnp.concatenate([smooth[:, :C], smooth[:, C:]], axis=0)
            noise = nbuf[pl.ds(2 * pair, 2), l].reshape(2 * NX, C)
            pre = dot(jnp.concatenate([smooth.astype(BF16), noise], axis=1), wcat[...])
            one = silu(pre + bias[...]).astype(BF16)
            two = silu(dot(one, wmid[...])).astype(BF16)
            new = (smooth + dot(two, wout[...])).astype(BF16)
            obuf[pl.ds(2 * pair, 2), l] = new.reshape(2, NX, C)
            return carry
        with jax.named_scope("G"):
            for l in range(l0, l0 + nl):
                lax.fori_loop(0, 2, functools.partial(column, l), 0)

        def moments(g, carry):
            lats = pl.ds(l0, nl)
            vals = [obuf[b, lats, pl.ds(MX * g, MX), :].astype(F32) for b in range(NB)]
            total = (vals[0] + vals[1]) + (vals[2] + vals[3])
            mean = total * (1.0 / NB)
            offs = [v - mean for v in vals]
            square = (offs[0] * offs[0] + offs[1] * offs[1]) + (offs[2] * offs[2] + offs[3] * offs[3])
            x, c = g // 2, lax.rem(g, 2)
            msend[lats, c, x, 0] = total.astype(BF16)
            msend[lats, c, x, 1] = square.astype(BF16)
            return carry
        with jax.named_scope("mom"):
            lax.fori_loop(0, NG, moments, 0)
        lats = pl.ds(l0, nl)
        pltpu.make_async_remote_copy(
            src_ref=msend.at[lats, 1 - mc], dst_ref=hrecv.at[lats],
            send_sem=h_ss.at[q], recv_sem=h_rs.at[q],
            device_id={"grp": mx * 2 + 1 - mc}, device_id_type=MESH).start()
        join(q)
        if q >= 1:
            combine(q - 1)
    combine(NQ - 1)
    for q in range(NQ):
        finish(q)

    with jax.named_scope("end"):
        @pl.when(source)
        def _():
            all_bytes(lsend.at[pl.ds(0, NT - 1)], l_ss)
        all_bytes(lrecv.at[pl.ds(0, NG - 1)], k_ss)
        all_bytes(qsend.at[pl.ds(0, NY - 1)], q_ss)
        all_bytes(t1send.at[pl.ds(0, NY - 1)], t1_ss)
        all_bytes(t3send.at[pl.ds(0, NY - 1)], t3_ss)
        for k in range(4):
            all_bytes(rp_send.at[k], rs_ss.at[0, k])
            all_bytes(fall.at[0], ag_ss.at[0, k])
            if k < 3:
                all_bytes(rm_send.at[k], rs_ss.at[1, k])
                all_bytes(fall.at[0], ag_ss.at[1, k])
        for pair in range(2):
            all_bytes(send1.at[pair, pl.ds(0, NT - 1)], s1_ss.at[pair])
            all_bytes(send2a.at[pair, pl.ds(0, NT - 1)], s2_ss.at[pair])
        for q, (l0, nl) in enumerate(CHUNKS):
            lats = pl.ds(l0, nl)
            if q > 0:
                all_bytes(send2b.at[pl.ds(l0 - 2, nl), pl.ds(0, NT - 1)], s2_ss.at[q + 1])
            all_bytes(hrecv.at[lats], h_ss.at[q])
            all_bytes(mrecv.at[lats, pl.ds(0, NX4 - 1)], m_ss.at[q])
            all_bytes(arecv.at[lats, pl.ds(0, NG - 1)], a_ss.at[q])


def write_out(o, m, v, new_h, mean_h, var_h, sem):
    copies = [pltpu.make_async_copy(s, d, sem.at[n])
              for n, (s, d) in enumerate(((o, new_h), (m, mean_h), (v, var_h)))]
    for c in copies:
        c.start()
    for c in copies:
        c.wait()


def per_device(grid_state, noise_field, legendre, diffusion, input_weight, noise_weight, input_bias,
               middle_weight, output_weight):
    hbm = pl.BlockSpec(memory_space=pltpu.HBM)
    vm = pl.BlockSpec(memory_space=pltpu.VMEM)
    dma = pltpu.SemaphoreType.DMA
    V = pltpu.VMEM
    shapes = (((NB, NL, NX, C), BF16), ((NL, NX, C), F32), ((NL, NX, C), F32))
    held = pl.pallas_call(
        kernel,
        out_shape=tuple(V(s, d) for s, d in shapes),
        in_specs=[hbm] * 9,
        out_specs=(vm, vm, vm),
        scratch_shapes=[
            V((NB, NL, NX, C), BF16), V((NB, NL, NX, C), BF16), V((NL, C, C), BF16), V((1, C), F32),
            V((H, H), BF16), V((1, H), F32), V((H, H), BF16), V((H, C), BF16),
            V((NT, NX), F32), V((NT, NX), F32), V((2 * C, NX), BF16), V((NX, 2 * C), BF16),
            V((NT, 4 * NL, C), BF16), V((NZ, NY, 4 * NL, C), BF16),
            V((NY, NL * NW, C), BF16), V((NY, NL * NW, C), BF16),
            V((2, NT, NL * 2 * J, C), BF16), V((2, NT, NL * 2 * J, C), BF16),
            V((2, NT, 4 * J, C), BF16), V((2, NT, 4 * J, C), BF16),
            V((NL - 2, NT, 4 * J, C), BF16), V((NL - 2, NT, 4 * J, C), BF16),
            V((NY, 2 * NB, NL * NW, C), BF16), V((NY, 2 * NB, NL * NW, C), BF16),
            V((NY, 2 * NB, NL * NW, C), BF16), V((NY, 2 * NB, NL * NW, C), BF16),
            V((NR, NY * NL * NW), BF16), V((NY * NL * NW, NR), BF16), V((NR, C), F32), V((2 * NB, NR, C), F32),
            V((4, NR, C), BF16), V((4, NR, C), BF16), V((3, NR, C), BF16), V((3, NR, C), BF16), V((NZ, NR, C), BF16),
            V((NT * NL * 2 * J, C), F32), V((NT * NL * 2 * J, C), F32),
            V((NL - 2, NT * 4 * J, C), F32), V((NT * 4 * J, C), F32),
            V((3, NT * NL, C), BF16), V((3, C, NT * NL), BF16), V((3, C, C), F32),
            V((NL, 2, NX4, 2, MX, C), BF16), V((NL, NX4, 2, MX, C), BF16),
            V((NL, NX4, 2, MX, C), BF16), V((NL, NX4, 2, MX, C), BF16),
            V((NL, 2, MX, C), BF16), V((NL, NG, 2, MX, C), BF16),
            dma((12,)), dma, dma, dma, dma, dma, dma, dma, dma, dma, dma,
            dma((2, 4)), dma((2, 4)), dma((2, 4)), dma((2, 4)),
            dma((2,)), dma((2,)), dma((NQ + 1,)), dma((NQ + 1,)),
            dma((NQ,)), dma((NQ,)), dma((NQ,)), dma((NQ,)), dma((NQ,)), dma((NQ,)),
        ],
        compiler_params=pltpu.CompilerParams(
            collective_id=0, has_side_effects=True, vmem_limit_bytes=48 * 1024 * 1024),
    )(*[pltpu.with_memory_space_constraint(a, pltpu.HBM) for a in (
        grid_state, noise_field, legendre, diffusion[None, :], input_weight, noise_weight, input_bias[None, :],
        middle_weight, output_weight)])
    return pl.pallas_call(
        write_out,
        out_shape=tuple(jax.ShapeDtypeStruct(s, d) for s, d in shapes),
        in_specs=[vm] * 3,
        out_specs=(hbm,) * 3,
        scratch_shapes=[dma((3,))],
        compiler_params=pltpu.CompilerParams(vmem_limit_bytes=1024 * 1024),
    )(*[pltpu.with_memory_space_constraint(a, pltpu.VMEM) for a in held])

def solution(mesh):
    in_specs = (P("grp", "lat", None, None), P("grp", "lat", None, None), P("lat", None, None)) + (P(),) * 6
    out_specs = (P("grp", "lat", None, None), P("lat", None, None), P("lat", None, None))
    return jax.shard_map(per_device, mesh=mesh, in_specs=in_specs, out_specs=out_specs, check_vma=False)
```

```python
import functools
import math

import jax
import jax.numpy as jnp
from jax import lax
from jax.experimental import pallas as pl
from jax.experimental.pallas import tpu as pltpu
from jax.sharding import PartitionSpec as P

MESH = pl.DeviceIdType.MESH
F32 = jnp.float32
BF16 = jnp.bfloat16

NY, NZ = 4, 8
NT = NY * NZ
NX4 = 4
NG = 8
NB = 4
NP = 2
NL = 6
NX = 384
C = 128
H = 256
MX = NX // NG
CHUNKS = ((0, 2), (2, 1), (3, 1), (4, 1), (5, 1))
NQ = len(CHUNKS)
MATES = ((2, 0), (2, 1), (1, 0), (3, 0), (1, 1), (3, 1), (0, 1))
LINE = (2, 1, 3)
J = 6
NW = 8
OFFS = (0, 32, 60, 84, 104, 120, 132, 140)
NR = 144


def dot(a, b):
    return jnp.dot(a, b, preferred_element_type=F32)


def silu(v):
    u = 0.5 * v
    return u + u * jnp.tanh(u)


def angle(lon, wave):
    return lax.rem(lon * wave, NX).astype(F32) * (2.0 * math.pi / NX)


def all_bytes(ref, sem):
    pltpu.make_async_copy(ref, ref, sem).wait()


def band_column(col):
    wave = jnp.zeros_like(col)
    start = jnp.zeros_like(col)
    for w in range(1, NW):
        wave = wave + jnp.where(col >= OFFS[w], 1, 0)
        start = start + jnp.where(col >= OFFS[w], OFFS[w] - OFFS[w - 1], 0)
    return wave, col - start + NY * wave


def kernel(
    grid_h, noise_h, leg_h, diff_h, win_h, wnoise_h, bias_h, wmid_h, wout_h,
    obuf, mbuf, vbuf,
    gbuf, nbuf, leg, diff, wcat, bias, wmid, wout, cosa, sina, tf, ti,
    lsend, lrecv, qsend, qrecv, send1, recv1, send2a, recv2a, send2b, recv2b,
    t1send, t1recv, t3send, t3recv, dmat, dtm, scale3, rf, rs_send, rs_recv, fall,
    zf, work_a, work_b, work_c, pn, pt, dm,
    msend, hrecv, csend, mrecv, asend, arecv,
    in_sem, l_ss, l_rs, k_ss, k_rs, q_ss, q_rs, t1_ss, t1_rs, t3_ss, t3_rs, rs_ss, rs_rs,
    s1_ss, s1_rs, s2_ss, s2_rs, h_ss, h_rs, m_ss, m_rs, a_ss, a_rs, b_ss, b_rs,
):
    lat, mg = lax.axis_index("lat"), lax.axis_index("grp")
    my, mz = lat // NZ, lax.rem(lat, NZ)
    me = mz * NY + my
    mx, mc = mg // 2, lax.rem(mg, 2)
    iota = lambda shape, dim: lax.broadcasted_iota(jnp.int32, shape, dim)

    def visit(j, dy, body):
        half = (j + 1) // 2
        dz = jnp.where(lax.rem(j, 2) == 1, NZ - half, half)
        y, z = lax.rem(my + dy, NY), lax.rem(mz + dz, NZ)
        body(y * NZ + z, z * NY + y)

    def each_peer(body):
        def step(n, carry):
            k = NT - n
            visit(k // NY, lax.rem(k, NY), body)
            return carry
        lax.fori_loop(1, NT, step, 0)

    def each_row(dy, body):
        def step(n, carry):
            visit(NZ - 1 - n, dy, body)
            return carry
        lax.fori_loop(0, NZ - (1 if dy == 0 else 0), step, 0)

    def each_mate(body):
        for dx, dc in MATES:
            body(lax.rem(mx + dx, NX4) * 2 + lax.rem(mc + dc, 2))

    def each_y(body):
        for dy in (2, 1, 3):
            y = lax.rem(my + dy, NY)
            body(y, y * NZ + mz)

    def around(d):
        return lax.rem(mz + d + NZ, NZ)

    def send(src, dst, ss, rs, lat_id):
        pltpu.make_async_remote_copy(
            src_ref=src, dst_ref=dst, send_sem=ss, recv_sem=rs,
            device_id={"lat": lat_id}, device_id_type=MESH).start()

    turn = 1 - 2 * mc

    def at(d):
        return my * NZ + around(turn * d)

    loads = [
        (grid_h.at[0], gbuf.at[0]), (grid_h.at[1], gbuf.at[1]), (grid_h.at[2], gbuf.at[2]), (grid_h.at[3], gbuf.at[3]),
        (leg_h, leg), (diff_h, diff), (win_h, wcat.at[pl.ds(0, C)]), (wnoise_h, wcat.at[pl.ds(C, C)]),
        (bias_h, bias), (wmid_h, wmid), (wout_h, wout), (noise_h, nbuf),
    ]
    loads = [pltpu.make_async_copy(s, d, in_sem.at[n]) for n, (s, d) in enumerate(loads)]
    loads[0].start()
    loads[1].start()
    barrier = pltpu.get_barrier_semaphore()
    each_peer(lambda t, s: pl.semaphore_signal(
        barrier, inc=1, device_id={"lat": t}, device_id_type=MESH))
    each_mate(lambda g: pl.semaphore_signal(
        barrier, inc=1, device_id={"grp": g}, device_id_type=MESH))
    for c in loads[2:]:
        c.start()

    with jax.named_scope("tables"):
        base = angle(iota((NT, NX), 1), iota((NT, NX), 0))
        cosa[...] = jnp.cos(base)
        sina[...] = jnp.sin(base)
        part = iota((8, NX), 0)
        step = angle(iota((8, NX), 1), NT * lax.rem(part, 4))
        scale = math.sqrt(2.0 / NX)
        cosb, sinb = scale * jnp.cos(step), scale * jnp.sin(step)
        real = part < 4
        u, v = jnp.where(real, cosb, -sinb), jnp.where(real, -sinb, -cosb)
        for j in range(J):
            k = 4 * (j // 3) + j % 3
            tf[pl.ds(NT * j, NT), :] = (cosa[...] * u[k:k + 1] + sina[...] * v[k:k + 1]).astype(BF16)
        row = iota((NT, NX), 0)
        high = angle(iota((NT, NX), 1), NY * lax.rem(row, NW) + row // NW)
        cosq, sinq = jnp.cos(high), jnp.sin(high)
        for q in range(NY):
            co, si = cosq[NW * q:NW * (q + 1)], sinq[NW * q:NW * (q + 1)]
            pair = [co * u[k:k + 1] + si * v[k:k + 1] for k in (3, 7)]
            tf[pl.ds(J * NT + 16 * q, 16), :] = jnp.concatenate(pair, axis=0).astype(BF16)

    def forward(b):
        loads[b].wait()
        for n in range(NL // 2):
            rhs = jnp.concatenate([gbuf[b, 2 * n], gbuf[b, 2 * n + 1]], axis=1)
            out = dot(tf[...], rhs)
            high = []
            for k in range(2):
                lanes = out[:, k * C:(k + 1) * C]
                for j in range(J):
                    zf[pl.ds((2 * n + k) * 2 * J + (b % 2) * J + j, NT, stride=NL * 2 * J), :] = (
                        lanes[NT * j:NT * (j + 1)])
                high.append(lanes[J * NT:].reshape(NY, 2, NW, C))
            high = jnp.concatenate(high, axis=2).astype(BF16)
            for r in range(2):
                t1send[:, r * NB + b, pl.ds(16 * n, 16), :] = high[:, r]

    def pack(pair):
        send1[pair] = zf[...].astype(BF16).reshape(NT, NL * 2 * J, C)
        recv1[pair, me] = send1[pair, me]

    def send_first(pair, dy):
        each_row(dy, lambda t, s: send(
            send1.at[pair, s], recv1.at[pair, me], s1_ss.at[pair], s1_rs.at[pair], t))

    with jax.named_scope("F"):
        forward(0)
        forward(1)
        pack(0)
        forward(2)
        forward(3)
        pack(1)
    loads[4].wait()
    source = mz == mg
    with jax.named_scope("basis"):
        work_a[pl.ds(0, NL * C), :] = leg[...].astype(F32).reshape(NL * C, C)
        for q in range(NY):
            band = [work_a[pl.ds(C * l + 3 * NT + q, NW, stride=NY), :] for l in range(NL)]
            qsend[q] = jnp.concatenate(band, axis=0).astype(BF16)

        @pl.when(source)
        def _():
            def pack_leg(p, carry):
                lsend[p] = work_a[pl.ds(p, 4 * NL, stride=NT), :].astype(BF16)
                return carry
            lax.fori_loop(0, NT, pack_leg, 0)

    with jax.named_scope("barrier"):
        pl.semaphore_wait(barrier, NT - 1 + NG - 1)

    send_first(0, 0)
    each_y(lambda y, t: send(qsend.at[y], qrecv.at[my], q_ss, q_rs, t))
    each_y(lambda y, t: send(t1send.at[y], t1recv.at[my], t1_ss, t1_rs, t))

    @pl.when(source)
    def _():
        each_peer(lambda t, s: send(lsend.at[s], lrecv.at[mz, my], l_ss, l_rs, t))
        lrecv[mz, my] = lsend[me]
    send_first(1, 0)
    qrecv[my] = qsend[my]
    t1recv[my] = t1send[my]
    with jax.named_scope("prep"):
        loads[5].wait()
        rows = iota((C, C), 0)

        def damp_at(degree):
            ratio = degree.astype(F32) * (degree.astype(F32) + 1.0) / float((C - 1) * C)
            return 1.0 / (1.0 + diff[...] * (ratio * ratio))
        damp = damp_at(rows)
        for i in range(3):
            dm[i] = jnp.where(rows >= me + NT * i, damp, 0.0)
        wave, degree = band_column(iota((NR, C), 0))
        scale3[...] = jnp.where(degree >= NY * wave + my, damp_at(degree + 3 * NT), 0.0)
    with jax.named_scope("w_q"):
        all_bytes(qrecv.at[pl.ds(0, NY - 1)], q_rs)
    with jax.named_scope("dmat"):
        col = iota((C, 2 * C), 1)
        _, degree = band_column(col)
        pick = jnp.where((col < NR) & (iota((C, 2 * C), 0) == degree + 3 * NT), 1.0, 0.0).astype(BF16)
        spread = dot(qrecv[...].reshape(NY * NL * NW, C), pick)
        wave, _ = band_column(iota((NY * NL * NW, 2 * C), 1))
        spread = jnp.where(lax.rem(iota((NY * NL * NW, 2 * C), 0), NW) == wave, spread, 0.0)
        dtm[...] = spread[:, :NR].astype(BF16)
        dmat[...] = spread.T[:NR].astype(BF16)
    with jax.named_scope("w_t1"):
        all_bytes(t1recv.at[pl.ds(0, NY - 1)], t1_rs)
    with jax.named_scope("R"):
        for k in range(0, 8, 2):
            both = [t1recv[:, k + e].reshape(NY * NL * NW, C) for e in range(2)]
            out = dot(dmat[...], jnp.concatenate(both, axis=1))
            rf[k] = out[:, :C]
            rf[k + 1] = out[:, C:]

    def ring_send(n, src, dst, hop):
        send(src, dst, rs_ss.at[n], rs_rs.at[n], at(hop))

    def ring_wait(*ids):
        for n in ids:
            all_bytes(fall.at[0], rs_rs.at[n])

    for n, (dest, hop) in enumerate(((4, 2), (3, 1), (-3, -1), (1, 1), (-1, -1))):
        rs_send[n] = rf[around(turn * dest)].astype(BF16)
    for n, (dest, hop) in enumerate(((4, 2), (3, 1), (-3, -1), (1, 1), (-1, -1))):
        ring_send(n, rs_send.at[n], rs_recv.at[n], hop)
    send_first(0, 1)
    send_first(0, 2)
    with jax.named_scope("prep2"):
        ti[...] = tf[...].astype(F32).T.astype(BF16)
    with jax.named_scope("w_rsA"):
        ring_wait(0, 1, 2)
    rs_send[5] = (rf[around(turn * 2)] + rs_recv[0].astype(F32) + rs_recv[1].astype(F32)).astype(BF16)
    rs_send[6] = (rf[around(turn * -2)] + rs_recv[2].astype(F32)).astype(BF16)
    ring_send(5, rs_send.at[5], rs_recv.at[5], 2)
    ring_send(6, rs_send.at[6], rs_recv.at[6], -2)
    send_first(0, 3)
    with jax.named_scope("w_leg"):
        @pl.when(source)
        def _():
            all_bytes(lrecv.at[mg, pl.ds(0, NY - 1)], l_rs)

        @pl.when(jnp.logical_not(source))
        def _():
            all_bytes(lrecv.at[mg], l_rs)
    each_mate(lambda g: pltpu.make_async_remote_copy(
        src_ref=lrecv.at[mg], dst_ref=lrecv.at[mg],
        send_sem=k_ss, recv_sem=k_rs, device_id={"grp": g}, device_id_type=MESH).start())
    with jax.named_scope("w_rsB"):
        ring_wait(3, 4, 5, 6)
    total = rf[mz]
    for n in range(3, 7):
        total += rs_recv[n].astype(F32)
    fall[mz] = (total * scale3[...]).astype(BF16)
    for n, hop in enumerate((2, -2, 1, -1)):
        ring_send(7 + n, fall.at[mz], fall.at[mz], hop)
    send_first(1, 1)
    with jax.named_scope("w_k"):
        all_bytes(lrecv.at[pl.ds(0, NG - 1)], k_rs)
    with jax.named_scope("prepP"):
        work_a[pl.ds(0, NT * 4 * NL), :] = lrecv[...].astype(F32).reshape(NT * 4 * NL, C)
        for i in range(3):
            basis = jnp.concatenate(
                [work_a[pl.ds(4 * l + i, NT, stride=4 * NL), :] for l in range(NL)], axis=0)
            pn[i] = basis.astype(BF16)
            pt[i] = basis.T.astype(BF16)

    def analyse(pair):
        with jax.named_scope("w_a1"):
            all_bytes(recv1.at[pair, pl.ds(0, NT - 1)], s1_rs.at[pair])

        def member(k, carry):
            for i in range(3):
                halves = [jnp.concatenate(
                    [work_a[pl.ds(2 * J * l + J * k + 3 * r + i, NT, stride=NL * 2 * J), :] for l in range(NL)],
                    axis=0).astype(BF16) for r in range(2)]
                spec = dot(pt[i], jnp.concatenate(halves, axis=1))
                scale = dm[i]
                filt = (spec * jnp.concatenate([scale, scale], axis=1)).astype(BF16)
                back = dot(pn[i], filt)
                for r in range(2):
                    j = 3 * r + i
                    for l in range(NL):
                        rows = back[NT * l:NT * (l + 1), r * C:(r + 1) * C]
                        if l < 2:
                            work_c[pl.ds(2 * J * l + J * k + j, NT, stride=4 * J), :] = rows
                        else:
                            work_b[l - 2, pl.ds(2 * J * pair + J * k + j, NT, stride=4 * J), :] = rows
            return carry
        with jax.named_scope("S"):
            work_a[...] = recv1[pair].astype(F32).reshape(NT * NL * 2 * J, C)
            lax.fori_loop(0, 2, member, 0)
            send2a[pair] = work_c[...].astype(BF16).reshape(NT, 4 * J, C)
            if pair == 1:
                for l in range(NL - 2):
                    send2b[l] = work_b[l].astype(BF16).reshape(NT, 4 * J, C)
        each_peer(lambda t, s: send(send2a.at[pair, s], recv2a.at[pair, me], s2_ss.at[pair], s2_rs.at[pair], t))
        recv2a[pair, me] = send2a[pair, me]

    with jax.named_scope("w_agA"):
        ring_wait(7, 8)
    behind, ahead = around(turn * -2), around(turn * 2)
    ring_send(11, fall.at[behind], fall.at[behind], 2)
    ring_send(12, fall.at[behind], fall.at[behind], 1)
    ring_send(13, fall.at[ahead], fall.at[ahead], -1)
    send_first(1, 2)
    send_first(1, 3)
    analyse(0)
    analyse(1)
    with jax.named_scope("w_agB"):
        ring_wait(9, 10, 11, 12, 13)
    with jax.named_scope("synth"):
        for k in range(0, 8, 2):
            out = dot(dtm[...], jnp.concatenate([fall[k], fall[k + 1]], axis=1)).astype(BF16)
            t3send[:, k] = out[:, :C].reshape(NY, NL * NW, C)
            t3send[:, k + 1] = out[:, C:].reshape(NY, NL * NW, C)
    for n in range(NL // 2):
        rows = pl.ds(16 * n, 16)
        each_y(lambda y, t: send(
            t3send.at[y, :, rows], t3recv.at[my, :, rows], t3_ss.at[n], t3_rs.at[n], t))
    with jax.named_scope("s2b"):
        for q in range(1, NQ):
            l0, nl = CHUNKS[q]
            lats = pl.ds(l0 - 2, nl)
            each_peer(lambda t, s: send(
                send2b.at[lats, s], recv2b.at[lats, me], s2_ss.at[q + 1], s2_rs.at[q + 1], t))
    t3recv[my] = t3send[my]
    for l in range(NL - 2):
        recv2b[l, me] = send2b[l, me]

    def join(q):
        l0, nl = CHUNKS[q]
        lats = pl.ds(l0, nl)
        with jax.named_scope("w_h"):
            all_bytes(hrecv.at[lats], h_rs.at[q])

        def one(x, carry):
            mine, theirs = msend[lats, mc, x, 0].astype(F32), hrecv[lats, x, 0].astype(F32)
            off = mine - theirs
            square = msend[lats, mc, x, 1].astype(F32) + hrecv[lats, x, 1].astype(F32)
            csend[lats, x, 0] = (mine + theirs).astype(BF16)
            csend[lats, x, 1] = (square + off * off * (1.0 / (2 * NB))).astype(BF16)
            return carry
        lax.fori_loop(0, NX4, one, 0)
        for dx in LINE:
            x = lax.rem(mx + dx, NX4)
            pltpu.make_async_remote_copy(
                src_ref=csend.at[lats, x], dst_ref=mrecv.at[lats, mx],
                send_sem=m_ss.at[q], recv_sem=m_rs.at[q],
                device_id={"grp": x * 2 + mc}, device_id_type=MESH).start()
        mrecv[lats, mx] = csend[lats, mx]

    def combine(q):
        l0, nl = CHUNKS[q]
        with jax.named_scope("w_m"):
            all_bytes(mrecv.at[pl.ds(l0, nl), pl.ds(0, NX4 - 1)], m_rs.at[q])
        lats = pl.ds(l0, nl)
        total = mrecv[lats, 0, 0].astype(F32)
        square = mrecv[lats, 0, 1].astype(F32)
        for x in range(1, NX4):
            total += mrecv[lats, x, 0].astype(F32)
            square += mrecv[lats, x, 1].astype(F32)
        mean = total * (1.0 / (NB * NG))
        for x in range(NX4):
            off = mrecv[lats, x, 0].astype(F32) * (1.0 / (2 * NB)) - mean
            square += (2 * NB) * (off * off)
        asend[lats, 0] = mean.astype(BF16)
        asend[lats, 1] = (square * (1.0 / (NB * NG - 1))).astype(BF16)
        for dx in LINE:
            pltpu.make_async_remote_copy(
                src_ref=asend.at[lats], dst_ref=arecv.at[lats, mc, mx],
                send_sem=a_ss.at[q], recv_sem=a_rs.at[q],
                device_id={"grp": lax.rem(mx + dx, NX4) * 2 + mc}, device_id_type=MESH).start()
        arecv[lats, mc, mx] = asend[lats]

    def spread(q):
        l0, nl = CHUNKS[q]
        lats = pl.ds(l0, nl)
        with jax.named_scope("w_ag"):
            all_bytes(mrecv.at[lats, pl.ds(0, NX4 - 1)], a_rs.at[q])
        pltpu.make_async_remote_copy(
            src_ref=arecv.at[lats, mc], dst_ref=arecv.at[lats, mc],
            send_sem=b_ss.at[q], recv_sem=b_rs.at[q],
            device_id={"grp": mx * 2 + 1 - mc}, device_id_type=MESH).start()

    def finish(q):
        l0, nl = CHUNKS[q]
        lats = pl.ds(l0, nl)
        with jax.named_scope("w_b"):
            all_bytes(hrecv.at[lats], b_rs.at[q])
        for g in range(NG):
            mbuf[lats, pl.ds(MX * g, MX), :] = arecv[lats, g % 2, g // 2, 0].astype(F32)
            vbuf[lats, pl.ds(MX * g, MX), :] = arecv[lats, g % 2, g // 2, 1].astype(F32)

    for c in loads[6:]:
        c.wait()
    for q, (l0, nl) in enumerate(CHUNKS):
        if l0 % 2 == 0:
            with jax.named_scope("w_t3"):
                all_bytes(t3recv.at[pl.ds(0, NY - 1), :, pl.ds(8 * l0, 16)], t3_rs.at[l0 // 2])
        with jax.named_scope("w_a2"):
            if q == 0:
                for pair in range(2):
                    all_bytes(recv2a.at[pair, pl.ds(0, NT - 1)], s2_rs.at[pair])
            else:
                all_bytes(recv2b.at[pl.ds(l0 - 2, nl), pl.ds(0, NT - 1)], s2_rs.at[q + 1])

        def column(l, pair, carry):
            if l < 2:
                work_c[...] = recv2a[pair].astype(F32).reshape(NT * 4 * J, C)
                first = 2 * J * l
            else:
                work_c[...] = recv2b[l - 2].astype(F32).reshape(NT * 4 * J, C)
                first = 2 * J * pair
            sides = []
            for k in range(2):
                rows = [work_c[pl.ds(first + J * k + j, NT, stride=4 * J), :] for j in range(J)]
                for y in range(NY):
                    for r in range(2):
                        two = t3recv[y, r * NB + 2 * pair + k, pl.ds(16 * (l // 2), 16), :].astype(F32)
                        rows.append(two[8 * (l % 2):8 * (l % 2) + 8])
                sides.append(jnp.concatenate(rows, axis=0).astype(BF16))
            smooth = dot(ti[...], jnp.concatenate(sides, axis=1))
            smooth = jnp.concatenate([smooth[:, :C], smooth[:, C:]], axis=0)
            noise = nbuf[pl.ds(2 * pair, 2), l].reshape(2 * NX, C)
            pre = dot(jnp.concatenate([smooth.astype(BF16), noise], axis=1), wcat[...])
            one = silu(pre + bias[...]).astype(BF16)
            two = silu(dot(one, wmid[...])).astype(BF16)
            new = (smooth + dot(two, wout[...])).astype(BF16)
            obuf[pl.ds(2 * pair, 2), l] = new.reshape(2, NX, C)
            return carry
        with jax.named_scope("G"):
            for l in range(l0, l0 + nl):
                lax.fori_loop(0, 2, functools.partial(column, l), 0)

        def moments(g, carry):
            lats = pl.ds(l0, nl)
            vals = [obuf[b, lats, pl.ds(MX * g, MX), :].astype(F32) for b in range(NB)]
            total = (vals[0] + vals[1]) + (vals[2] + vals[3])
            mean = total * (1.0 / NB)
            offs = [v - mean for v in vals]
            square = (offs[0] * offs[0] + offs[1] * offs[1]) + (offs[2] * offs[2] + offs[3] * offs[3])
            x, c = g // 2, lax.rem(g, 2)
            msend[lats, c, x, 0] = total.astype(BF16)
            msend[lats, c, x, 1] = square.astype(BF16)
            return carry
        with jax.named_scope("mom"):
            lax.fori_loop(0, NG, moments, 0)
        lats = pl.ds(l0, nl)
        pltpu.make_async_remote_copy(
            src_ref=msend.at[lats, 1 - mc], dst_ref=hrecv.at[lats],
            send_sem=h_ss.at[q], recv_sem=h_rs.at[q],
            device_id={"grp": mx * 2 + 1 - mc}, device_id_type=MESH).start()
        join(q)
        if q >= 1:
            combine(q - 1)
        if q >= 3:
            spread(q - 3)
    spread(NQ - 3)
    for q in range(NQ - 3):
        finish(q)
    combine(NQ - 1)
    spread(NQ - 2)
    spread(NQ - 1)
    for q in range(NQ - 3, NQ):
        finish(q)

    with jax.named_scope("end"):
        @pl.when(source)
        def _():
            all_bytes(lsend.at[pl.ds(0, NT - 1)], l_ss)
        all_bytes(lrecv.at[pl.ds(0, NG - 1)], k_ss)
        all_bytes(qsend.at[pl.ds(0, NY - 1)], q_ss)
        all_bytes(t1send.at[pl.ds(0, NY - 1)], t1_ss)
        for n in range(NL // 2):
            all_bytes(t3send.at[pl.ds(0, NY - 1), :, pl.ds(16 * n, 16)], t3_ss.at[n])
        for n in range(14):
            all_bytes(fall.at[0], rs_ss.at[n])
        for pair in range(2):
            all_bytes(send1.at[pair, pl.ds(0, NT - 1)], s1_ss.at[pair])
            all_bytes(send2a.at[pair, pl.ds(0, NT - 1)], s2_ss.at[pair])
        for q, (l0, nl) in enumerate(CHUNKS):
            lats = pl.ds(l0, nl)
            if q > 0:
                all_bytes(send2b.at[pl.ds(l0 - 2, nl), pl.ds(0, NT - 1)], s2_ss.at[q + 1])
            all_bytes(hrecv.at[lats], h_ss.at[q])
            all_bytes(mrecv.at[lats, pl.ds(0, NX4 - 1)], m_ss.at[q])
            all_bytes(mrecv.at[lats, pl.ds(0, NX4 - 1)], a_ss.at[q])
            all_bytes(hrecv.at[lats], b_ss.at[q])


def write_out(o, m, v, new_h, mean_h, var_h, sem):
    pieces = [(o.at[b], new_h.at[b]) for b in range(NB)]
    for n in range(2):
        half = pl.ds(n * (NL // 2), NL // 2)
        pieces += [(m.at[half], mean_h.at[half]), (v.at[half], var_h.at[half])]
    copies = [pltpu.make_async_copy(s, d, sem.at[n]) for n, (s, d) in enumerate(pieces)]
    for c in copies:
        c.start()
    for c in copies:
        c.wait()


def per_device(grid_state, noise_field, legendre, diffusion, input_weight, noise_weight, input_bias,
               middle_weight, output_weight):
    hbm = pl.BlockSpec(memory_space=pltpu.HBM)
    vm = pl.BlockSpec(memory_space=pltpu.VMEM)
    dma = pltpu.SemaphoreType.DMA
    V = pltpu.VMEM
    shapes = (((NB, NL, NX, C), BF16), ((NL, NX, C), F32), ((NL, NX, C), F32))
    held = pl.pallas_call(
        kernel,
        out_shape=tuple(V(s, d) for s, d in shapes),
        in_specs=[hbm] * 9,
        out_specs=(vm, vm, vm),
        scratch_shapes=[
            V((NB, NL, NX, C), BF16), V((NB, NL, NX, C), BF16), V((NL, C, C), BF16), V((1, C), F32),
            V((H, H), BF16), V((1, H), F32), V((H, H), BF16), V((H, C), BF16),
            V((NT, NX), F32), V((NT, NX), F32), V((2 * C, NX), BF16), V((NX, 2 * C), BF16),
            V((NT, 4 * NL, C), BF16), V((NZ, NY, 4 * NL, C), BF16),
            V((NY, NL * NW, C), BF16), V((NY, NL * NW, C), BF16),
            V((2, NT, NL * 2 * J, C), BF16), V((2, NT, NL * 2 * J, C), BF16),
            V((2, NT, 4 * J, C), BF16), V((2, NT, 4 * J, C), BF16),
            V((NL - 2, NT, 4 * J, C), BF16), V((NL - 2, NT, 4 * J, C), BF16),
            V((NY, 2 * NB, NL * NW, C), BF16), V((NY, 2 * NB, NL * NW, C), BF16),
            V((NY, 2 * NB, NL * NW, C), BF16), V((NY, 2 * NB, NL * NW, C), BF16),
            V((NR, NY * NL * NW), BF16), V((NY * NL * NW, NR), BF16), V((NR, C), F32), V((2 * NB, NR, C), F32),
            V((7, NR, C), BF16), V((7, NR, C), BF16), V((NZ, NR, C), BF16),
            V((NT * NL * 2 * J, C), F32), V((NT * NL * 2 * J, C), F32),
            V((NL - 2, NT * 4 * J, C), F32), V((NT * 4 * J, C), F32),
            V((3, NT * NL, C), BF16), V((3, C, NT * NL), BF16), V((3, C, C), F32),
            V((NL, 2, NX4, 2, MX, C), BF16), V((NL, NX4, 2, MX, C), BF16),
            V((NL, NX4, 2, MX, C), BF16), V((NL, NX4, 2, MX, C), BF16),
            V((NL, 2, MX, C), BF16), V((NL, 2, NX4, 2, MX, C), BF16),
            dma((12,)), dma, dma, dma, dma, dma, dma, dma, dma, dma((NL // 2,)), dma((NL // 2,)),
            dma((14,)), dma((14,)),
            dma((2,)), dma((2,)), dma((NQ + 1,)), dma((NQ + 1,)),
            dma((NQ,)), dma((NQ,)), dma((NQ,)), dma((NQ,)), dma((NQ,)), dma((NQ,)), dma((NQ,)), dma((NQ,)),
        ],
        compiler_params=pltpu.CompilerParams(
            collective_id=0, has_side_effects=True, vmem_limit_bytes=48 * 1024 * 1024),
    )(*[pltpu.with_memory_space_constraint(a, pltpu.HBM) for a in (
        grid_state, noise_field, legendre, diffusion[None, :], input_weight, noise_weight, input_bias[None, :],
        middle_weight, output_weight)])
    return pl.pallas_call(
        write_out,
        out_shape=tuple(jax.ShapeDtypeStruct(s, d) for s, d in shapes),
        in_specs=[vm] * 3,
        out_specs=(hbm,) * 3,
        scratch_shapes=[dma((8,))],
        compiler_params=pltpu.CompilerParams(vmem_limit_bytes=1024 * 1024),
    )(*[pltpu.with_memory_space_constraint(a, pltpu.VMEM) for a in held])

def solution(mesh):
    in_specs = (P("grp", "lat", None, None), P("grp", "lat", None, None), P("lat", None, None)) + (P(),) * 6
    out_specs = (P("grp", "lat", None, None), P("lat", None, None), P("lat", None, None))
    return jax.shard_map(per_device, mesh=mesh, in_specs=in_specs, out_specs=out_specs, check_vma=False)
```

```python
import math

import jax
import jax.numpy as jnp
from jax import lax
from jax.experimental import pallas as pl
from jax.experimental.pallas import tpu as pltpu
from jax.sharding import PartitionSpec as P

MESH = pl.DeviceIdType.MESH
F32 = jnp.float32
BF16 = jnp.bfloat16

NY, NZ = 4, 8
NT = NY * NZ
NX4 = 4
NG = 8
NB = 4
NP = 2
NL = 6
NX = 384
C = 128
H = 256
MX = NX // NG
CHUNKS = ((0, 2), (2, 1), (3, 1), (4, 1), (5, 1))
NQ = len(CHUNKS)
MATES = ((2, 0), (2, 1), (1, 0), (3, 0), (1, 1), (3, 1), (0, 1))
LINE = (2, 1, 3)
J = 6
NW = 8
OFFS = (0, 32, 60, 84, 104, 120, 132, 140)
NR = 144


def dot(a, b):
    return jnp.dot(a, b, preferred_element_type=F32)


def silu(v):
    u = 0.5 * v
    return u + u * jnp.tanh(u)


def angle(lon, wave):
    return lax.rem(lon * wave, NX).astype(F32) * (2.0 * math.pi / NX)


def all_bytes(ref, sem):
    pltpu.make_async_copy(ref, ref, sem).wait()


def band_column(col):
    wave = jnp.zeros_like(col)
    start = jnp.zeros_like(col)
    for w in range(1, NW):
        wave = wave + jnp.where(col >= OFFS[w], 1, 0)
        start = start + jnp.where(col >= OFFS[w], OFFS[w] - OFFS[w - 1], 0)
    return wave, col - start + NY * wave


def kernel(
    grid_h, noise_h, leg_h, diff_h, win_h, wnoise_h, bias_h, wmid_h, wout_h,
    obuf, mbuf, vbuf,
    gbuf, nbuf, leg, diff, wcat, bias, wmid, wout, cosa, sina, tf, ti,
    lsend, lrecv, qsend, qrecv, send1, recv1, send2a, recv2a, send2b, recv2b,
    t1send, t1recv, t3send, t3recv, dmat, dtm, scale3, rf, rs_send, rs_recv, fall,
    zf, work_a, work_b, work_c, pn, pt, dm,
    msend, hrecv, csend, mrecv, asend, arecv,
    in_sem, l_ss, l_rs, k_ss, k_rs, q_ss, q_rs, t1_ss, t1_rs, t3_ss, t3_rs, rs_ss, rs_rs,
    s1_ss, s1_rs, s2_ss, s2_rs, h_ss, h_rs, m_ss, m_rs, a_ss, a_rs, b_ss, b_rs,
):
    lat, mg = lax.axis_index("lat"), lax.axis_index("grp")
    my, mz = lat // NZ, lax.rem(lat, NZ)
    me = mz * NY + my
    mx, mc = mg // 2, lax.rem(mg, 2)
    iota = lambda shape, dim: lax.broadcasted_iota(jnp.int32, shape, dim)

    def visit(j, dy, body):
        half = (j + 1) // 2
        dz = jnp.where(lax.rem(j, 2) == 1, NZ - half, half)
        y, z = lax.rem(my + dy, NY), lax.rem(mz + dz, NZ)
        body(y * NZ + z, z * NY + y)

    def each_peer(body):
        def step(n, carry):
            k = NT - n
            visit(k // NY, lax.rem(k, NY), body)
            return carry
        lax.fori_loop(1, NT, step, 0)

    def each_row(dy, body):
        def step(n, carry):
            visit(NZ - 1 - n, dy, body)
            return carry
        lax.fori_loop(0, NZ - (1 if dy == 0 else 0), step, 0)

    def each_mate(body):
        for dx, dc in MATES:
            body(lax.rem(mx + dx, NX4) * 2 + lax.rem(mc + dc, 2))

    def each_y(body):
        for dy in (2, 1, 3):
            y = lax.rem(my + dy, NY)
            body(y, y * NZ + mz)

    def around(d):
        return lax.rem(mz + d + NZ, NZ)

    def send(src, dst, ss, rs, lat_id):
        pltpu.make_async_remote_copy(
            src_ref=src, dst_ref=dst, send_sem=ss, recv_sem=rs,
            device_id={"lat": lat_id}, device_id_type=MESH).start()

    turn = 1 - 2 * mc

    def at(d):
        return my * NZ + around(turn * d)

    loads = [
        (grid_h.at[0], gbuf.at[0]), (grid_h.at[1], gbuf.at[1]), (grid_h.at[2], gbuf.at[2]), (grid_h.at[3], gbuf.at[3]),
        (leg_h, leg), (diff_h, diff), (win_h, wcat.at[pl.ds(0, C)]), (wnoise_h, wcat.at[pl.ds(C, C)]),
        (bias_h, bias), (wmid_h, wmid), (wout_h, wout), (noise_h, nbuf),
    ]
    loads = [pltpu.make_async_copy(s, d, in_sem.at[n]) for n, (s, d) in enumerate(loads)]
    loads[0].start()
    loads[1].start()
    barrier = pltpu.get_barrier_semaphore()
    each_peer(lambda t, s: pl.semaphore_signal(
        barrier, inc=1, device_id={"lat": t}, device_id_type=MESH))
    each_mate(lambda g: pl.semaphore_signal(
        barrier, inc=1, device_id={"grp": g}, device_id_type=MESH))
    for c in loads[2:]:
        c.start()

    with jax.named_scope("tables"):
        base = angle(iota((NT, NX), 1), iota((NT, NX), 0))
        cosa[...] = jnp.cos(base)
        sina[...] = jnp.sin(base)
        part = iota((8, NX), 0)
        step = angle(iota((8, NX), 1), NT * lax.rem(part, 4))
        scale = math.sqrt(2.0 / NX)
        cosb, sinb = scale * jnp.cos(step), scale * jnp.sin(step)
        real = part < 4
        u, v = jnp.where(real, cosb, -sinb), jnp.where(real, -sinb, -cosb)
        for j in range(J):
            k = 4 * (j // 3) + j % 3
            tf[pl.ds(NT * j, NT), :] = (cosa[...] * u[k:k + 1] + sina[...] * v[k:k + 1]).astype(BF16)
        row = iota((NT, NX), 0)
        high = angle(iota((NT, NX), 1), NY * lax.rem(row, NW) + row // NW)
        cosq, sinq = jnp.cos(high), jnp.sin(high)
        for q in range(NY):
            co, si = cosq[NW * q:NW * (q + 1)], sinq[NW * q:NW * (q + 1)]
            pair = [co * u[k:k + 1] + si * v[k:k + 1] for k in (3, 7)]
            tf[pl.ds(J * NT + 16 * q, 16), :] = jnp.concatenate(pair, axis=0).astype(BF16)

    def forward(b):
        loads[b].wait()
        for n in range(NL // 2):
            rhs = jnp.concatenate([gbuf[b, 2 * n], gbuf[b, 2 * n + 1]], axis=1)
            out = dot(tf[...], rhs)
            high = []
            for k in range(2):
                lanes = out[:, k * C:(k + 1) * C]
                for j in range(J):
                    zf[pl.ds((2 * n + k) * 2 * J + (b % 2) * J + j, NT, stride=NL * 2 * J), :] = (
                        lanes[NT * j:NT * (j + 1)])
                high.append(lanes[J * NT:].reshape(NY, 2, NW, C))
            high = jnp.concatenate(high, axis=2).astype(BF16)
            for r in range(2):
                t1send[:, r * NB + b, pl.ds(16 * n, 16), :] = high[:, r]

    def pack(pair):
        send1[pair] = zf[...].astype(BF16).reshape(NT, NL * 2 * J, C)
        recv1[pair, me] = send1[pair, me]

    def send_first(pair, dy):
        each_row(dy, lambda t, s: send(
            send1.at[pair, s], recv1.at[pair, me], s1_ss.at[pair], s1_rs.at[pair], t))

    with jax.named_scope("F"):
        forward(0)
        forward(1)
        pack(0)
        forward(2)
        forward(3)
        pack(1)
    loads[4].wait()
    source = mz == mg
    with jax.named_scope("basis"):
        work_a[pl.ds(0, NL * C), :] = leg[...].astype(F32).reshape(NL * C, C)
        for q in range(NY):
            band = [work_a[pl.ds(C * l + 3 * NT + q, NW, stride=NY), :] for l in range(NL)]
            qsend[q] = jnp.concatenate(band, axis=0).astype(BF16)

        @pl.when(source)
        def _():
            def pack_leg(p, carry):
                lsend[p] = work_a[pl.ds(p, 4 * NL, stride=NT), :].astype(BF16)
                return carry
            lax.fori_loop(0, NT, pack_leg, 0)

    with jax.named_scope("barrier"):
        pl.semaphore_wait(barrier, NT - 1 + NG - 1)

    send_first(0, 0)
    each_y(lambda y, t: send(qsend.at[y], qrecv.at[my], q_ss, q_rs, t))
    each_y(lambda y, t: send(t1send.at[y], t1recv.at[my], t1_ss, t1_rs, t))

    @pl.when(source)
    def _():
        each_peer(lambda t, s: send(lsend.at[s], lrecv.at[mz, my], l_ss, l_rs, t))
        lrecv[mz, my] = lsend[me]
    send_first(1, 0)
    qrecv[my] = qsend[my]
    t1recv[my] = t1send[my]
    with jax.named_scope("prep"):
        loads[5].wait()
        rows = iota((C, C), 0)

        def damp_at(degree):
            ratio = degree.astype(F32) * (degree.astype(F32) + 1.0) / float((C - 1) * C)
            return 1.0 / (1.0 + diff[...] * (ratio * ratio))
        damp = damp_at(rows)
        for i in range(3):
            dm[i] = jnp.where(rows >= me + NT * i, damp, 0.0)
        wave, degree = band_column(iota((NR, C), 0))
        scale3[...] = jnp.where(degree >= NY * wave + my, damp_at(degree + 3 * NT), 0.0)
    with jax.named_scope("w_q"):
        all_bytes(qrecv.at[pl.ds(0, NY - 1)], q_rs)
    with jax.named_scope("dmat"):
        col = iota((C, 2 * C), 1)
        _, degree = band_column(col)
        pick = jnp.where((col < NR) & (iota((C, 2 * C), 0) == degree + 3 * NT), 1.0, 0.0).astype(BF16)
        spread = dot(qrecv[...].reshape(NY * NL * NW, C), pick)
        wave, _ = band_column(iota((NY * NL * NW, 2 * C), 1))
        spread = jnp.where(lax.rem(iota((NY * NL * NW, 2 * C), 0), NW) == wave, spread, 0.0)
        dtm[...] = spread[:, :NR].astype(BF16)
        dmat[...] = spread.T[:NR].astype(BF16)
    with jax.named_scope("w_t1"):
        all_bytes(t1recv.at[pl.ds(0, NY - 1)], t1_rs)
    with jax.named_scope("R"):
        for k in range(0, 8, 2):
            both = [t1recv[:, k + e].reshape(NY * NL * NW, C) for e in range(2)]
            out = dot(dmat[...], jnp.concatenate(both, axis=1))
            rf[k] = out[:, :C]
            rf[k + 1] = out[:, C:]

    def ring_send(n, src, dst, hop):
        send(src, dst, rs_ss.at[n], rs_rs.at[n], at(hop))

    def ring_wait(*ids):
        for n in ids:
            all_bytes(fall.at[0], rs_rs.at[n])

    for n, (dest, hop) in enumerate(((4, 2), (3, 1), (-3, -1), (1, 1), (-1, -1))):
        rs_send[n] = rf[around(turn * dest)].astype(BF16)
    for n, (dest, hop) in enumerate(((4, 2), (3, 1), (-3, -1), (1, 1), (-1, -1))):
        ring_send(n, rs_send.at[n], rs_recv.at[n], hop)
    send_first(0, 1)
    send_first(0, 2)
    with jax.named_scope("prep2"):
        ti[...] = tf[...].astype(F32).T.astype(BF16)
    with jax.named_scope("w_rsA"):
        ring_wait(0, 1, 2)
    rs_send[5] = (rf[around(turn * 2)] + rs_recv[0].astype(F32) + rs_recv[1].astype(F32)).astype(BF16)
    rs_send[6] = (rf[around(turn * -2)] + rs_recv[2].astype(F32)).astype(BF16)
    ring_send(5, rs_send.at[5], rs_recv.at[5], 2)
    ring_send(6, rs_send.at[6], rs_recv.at[6], -2)
    send_first(0, 3)
    with jax.named_scope("w_leg"):
        @pl.when(source)
        def _():
            all_bytes(lrecv.at[mg, pl.ds(0, NY - 1)], l_rs)

        @pl.when(jnp.logical_not(source))
        def _():
            all_bytes(lrecv.at[mg], l_rs)
    each_mate(lambda g: pltpu.make_async_remote_copy(
        src_ref=lrecv.at[mg], dst_ref=lrecv.at[mg],
        send_sem=k_ss, recv_sem=k_rs, device_id={"grp": g}, device_id_type=MESH).start())
    with jax.named_scope("w_rsB"):
        ring_wait(3, 4, 5, 6)
    total = rf[mz]
    for n in range(3, 7):
        total += rs_recv[n].astype(F32)
    fall[mz] = (total * scale3[...]).astype(BF16)
    for n, hop in enumerate((2, -2, 1, -1)):
        ring_send(7 + n, fall.at[mz], fall.at[mz], hop)
    send_first(1, 1)
    with jax.named_scope("w_k"):
        all_bytes(lrecv.at[pl.ds(0, NG - 1)], k_rs)
    with jax.named_scope("prepP"):
        work_a[pl.ds(0, NT * 4 * NL), :] = lrecv[...].astype(F32).reshape(NT * 4 * NL, C)
        for i in range(3):
            basis = jnp.concatenate(
                [work_a[pl.ds(4 * l + i, NT, stride=4 * NL), :] for l in range(NL)], axis=0)
            pn[i] = basis.astype(BF16)
            pt[i] = basis.T.astype(BF16)

    def analyse(pair):
        with jax.named_scope("w_a1"):
            all_bytes(recv1.at[pair, pl.ds(0, NT - 1)], s1_rs.at[pair])

        def member(k, carry):
            for i in range(3):
                halves = [jnp.concatenate(
                    [work_a[pl.ds(2 * J * l + J * k + 3 * r + i, NT, stride=NL * 2 * J), :] for l in range(NL)],
                    axis=0).astype(BF16) for r in range(2)]
                spec = dot(pt[i], jnp.concatenate(halves, axis=1))
                scale = dm[i]
                filt = (spec * jnp.concatenate([scale, scale], axis=1)).astype(BF16)
                back = dot(pn[i], filt)
                for r in range(2):
                    j = 3 * r + i
                    for l in range(NL):
                        rows = back[NT * l:NT * (l + 1), r * C:(r + 1) * C]
                        if l < 2:
                            work_c[pl.ds(2 * J * l + J * k + j, NT, stride=4 * J), :] = rows
                        else:
                            work_b[l - 2, pl.ds(2 * J * pair + J * k + j, NT, stride=4 * J), :] = rows
            return carry
        with jax.named_scope("S"):
            work_a[...] = recv1[pair].astype(F32).reshape(NT * NL * 2 * J, C)
            lax.fori_loop(0, 2, member, 0)
            send2a[pair] = work_c[...].astype(BF16).reshape(NT, 4 * J, C)
            if pair == 1:
                for l in range(NL - 2):
                    send2b[l] = work_b[l].astype(BF16).reshape(NT, 4 * J, C)
        each_peer(lambda t, s: send(send2a.at[pair, s], recv2a.at[pair, me], s2_ss.at[pair], s2_rs.at[pair], t))
        recv2a[pair, me] = send2a[pair, me]

    with jax.named_scope("w_agA"):
        ring_wait(7, 8)
    behind, ahead = around(turn * -2), around(turn * 2)
    ring_send(11, fall.at[behind], fall.at[behind], 2)
    ring_send(12, fall.at[behind], fall.at[behind], 1)
    ring_send(13, fall.at[ahead], fall.at[ahead], -1)
    send_first(1, 2)
    send_first(1, 3)
    analyse(0)
    analyse(1)
    with jax.named_scope("w_agB"):
        ring_wait(9, 10, 11, 12, 13)
    with jax.named_scope("synth"):
        for k in range(0, 8, 2):
            out = dot(dtm[...], jnp.concatenate([fall[k], fall[k + 1]], axis=1)).astype(BF16)
            t3send[:, k] = out[:, :C].reshape(NY, NL * NW, C)
            t3send[:, k + 1] = out[:, C:].reshape(NY, NL * NW, C)
    for n in range(NL // 2):
        rows = pl.ds(16 * n, 16)
        each_y(lambda y, t: send(
            t3send.at[y, :, rows], t3recv.at[my, :, rows], t3_ss.at[n], t3_rs.at[n], t))
    with jax.named_scope("s2b"):
        for q in range(1, NQ):
            l0, nl = CHUNKS[q]
            lats = pl.ds(l0 - 2, nl)
            each_peer(lambda t, s: send(
                send2b.at[lats, s], recv2b.at[lats, me], s2_ss.at[q + 1], s2_rs.at[q + 1], t))
    t3recv[my] = t3send[my]
    for l in range(NL - 2):
        recv2b[l, me] = send2b[l, me]

    def join(q):
        l0, nl = CHUNKS[q]
        lats = pl.ds(l0, nl)
        with jax.named_scope("w_h"):
            all_bytes(hrecv.at[lats], h_rs.at[q])

        def one(x, carry):
            mine, theirs = msend[lats, mc, x, 0].astype(F32), hrecv[lats, x, 0].astype(F32)
            off = mine - theirs
            square = msend[lats, mc, x, 1].astype(F32) + hrecv[lats, x, 1].astype(F32)
            csend[lats, x, 0] = (mine + theirs).astype(BF16)
            csend[lats, x, 1] = (square + off * off * (1.0 / (2 * NB))).astype(BF16)
            return carry
        lax.fori_loop(0, NX4, one, 0)
        for dx in LINE:
            x = lax.rem(mx + dx, NX4)
            pltpu.make_async_remote_copy(
                src_ref=csend.at[lats, x], dst_ref=mrecv.at[lats, mx],
                send_sem=m_ss.at[q], recv_sem=m_rs.at[q],
                device_id={"grp": x * 2 + mc}, device_id_type=MESH).start()
        mrecv[lats, mx] = csend[lats, mx]

    def combine(q):
        l0, nl = CHUNKS[q]
        with jax.named_scope("w_m"):
            all_bytes(mrecv.at[pl.ds(l0, nl), pl.ds(0, NX4 - 1)], m_rs.at[q])
        lats = pl.ds(l0, nl)
        total = mrecv[lats, 0, 0].astype(F32)
        square = mrecv[lats, 0, 1].astype(F32)
        for x in range(1, NX4):
            total += mrecv[lats, x, 0].astype(F32)
            square += mrecv[lats, x, 1].astype(F32)
        mean = total * (1.0 / (NB * NG))
        for x in range(NX4):
            off = mrecv[lats, x, 0].astype(F32) * (1.0 / (2 * NB)) - mean
            square += (2 * NB) * (off * off)
        asend[lats, 0] = mean.astype(BF16)
        asend[lats, 1] = (square * (1.0 / (NB * NG - 1))).astype(BF16)
        for dx in LINE:
            pltpu.make_async_remote_copy(
                src_ref=asend.at[lats], dst_ref=arecv.at[lats, mc, mx],
                send_sem=a_ss.at[q], recv_sem=a_rs.at[q],
                device_id={"grp": lax.rem(mx + dx, NX4) * 2 + mc}, device_id_type=MESH).start()
        arecv[lats, mc, mx] = asend[lats]

    def spread(q):
        l0, nl = CHUNKS[q]
        lats = pl.ds(l0, nl)
        with jax.named_scope("w_ag"):
            all_bytes(mrecv.at[lats, pl.ds(0, NX4 - 1)], a_rs.at[q])
        pltpu.make_async_remote_copy(
            src_ref=arecv.at[lats, mc], dst_ref=arecv.at[lats, mc],
            send_sem=b_ss.at[q], recv_sem=b_rs.at[q],
            device_id={"grp": mx * 2 + 1 - mc}, device_id_type=MESH).start()

    def finish(q):
        l0, nl = CHUNKS[q]
        lats = pl.ds(l0, nl)
        with jax.named_scope("w_b"):
            all_bytes(hrecv.at[lats], b_rs.at[q])
        for g in range(NG):
            mbuf[lats, pl.ds(MX * g, MX), :] = arecv[lats, g % 2, g // 2, 0].astype(F32)
            vbuf[lats, pl.ds(MX * g, MX), :] = arecv[lats, g % 2, g // 2, 1].astype(F32)

    for c in loads[6:]:
        c.wait()
    for q, (l0, nl) in enumerate(CHUNKS):
        if l0 % 2 == 0:
            with jax.named_scope("w_t3"):
                all_bytes(t3recv.at[pl.ds(0, NY - 1), :, pl.ds(8 * l0, 16)], t3_rs.at[l0 // 2])
        with jax.named_scope("w_a2"):
            if q == 0:
                for pair in range(2):
                    all_bytes(recv2a.at[pair, pl.ds(0, NT - 1)], s2_rs.at[pair])
            else:
                all_bytes(recv2b.at[pl.ds(l0 - 2, nl), pl.ds(0, NT - 1)], s2_rs.at[q + 1])

        def column(l, pair):
            area = work_a.at[pl.ds(pair * NT * 4 * J, NT * 4 * J)]
            if l < 2:
                area[...] = recv2a[pair].astype(F32).reshape(NT * 4 * J, C)
                first = 2 * J * l
            else:
                area[...] = recv2b[l - 2].astype(F32).reshape(NT * 4 * J, C)
                first = 2 * J * pair
            sides = []
            for k in range(2):
                rows = [area[pl.ds(first + J * k + j, NT, stride=4 * J), :] for j in range(J)]
                for y in range(NY):
                    for r in range(2):
                        two = t3recv[y, r * NB + 2 * pair + k, pl.ds(16 * (l // 2), 16), :].astype(F32)
                        rows.append(two[8 * (l % 2):8 * (l % 2) + 8])
                sides.append(jnp.concatenate(rows, axis=0).astype(BF16))
            smooth = dot(ti[...], jnp.concatenate(sides, axis=1))
            smooth = jnp.concatenate([smooth[:, :C], smooth[:, C:]], axis=0)
            noise = nbuf[pl.ds(2 * pair, 2), l].reshape(2 * NX, C)
            pre = dot(jnp.concatenate([smooth.astype(BF16), noise], axis=1), wcat[...])
            one = silu(pre + bias[...]).astype(BF16)
            two = silu(dot(one, wmid[...])).astype(BF16)
            new = (smooth + dot(two, wout[...])).astype(BF16)
            obuf[pl.ds(2 * pair, 2), l] = new.reshape(2, NX, C)
        with jax.named_scope("G"):
            for l in range(l0, l0 + nl):
                for pair in range(2):
                    column(l, pair)

        def moments(g, carry):
            lats = pl.ds(l0, nl)
            vals = [obuf[b, lats, pl.ds(MX * g, MX), :].astype(F32) for b in range(NB)]
            total = (vals[0] + vals[1]) + (vals[2] + vals[3])
            mean = total * (1.0 / NB)
            offs = [v - mean for v in vals]
            square = (offs[0] * offs[0] + offs[1] * offs[1]) + (offs[2] * offs[2] + offs[3] * offs[3])
            x, c = g // 2, lax.rem(g, 2)
            msend[lats, c, x, 0] = total.astype(BF16)
            msend[lats, c, x, 1] = square.astype(BF16)
            return carry
        with jax.named_scope("mom"):
            lax.fori_loop(0, NG, moments, 0)
        lats = pl.ds(l0, nl)
        pltpu.make_async_remote_copy(
            src_ref=msend.at[lats, 1 - mc], dst_ref=hrecv.at[lats],
            send_sem=h_ss.at[q], recv_sem=h_rs.at[q],
            device_id={"grp": mx * 2 + 1 - mc}, device_id_type=MESH).start()
        if 1 <= q < NQ - 1:
            join(q - 1)
        if 2 <= q < NQ - 1:
            combine(q - 2)
        if q >= NQ - 2:
            join(q)
    combine(NQ - 3)
    for q in range(NQ - 3):
        spread(q)
    for q in range(NQ - 3):
        finish(q)
    combine(NQ - 2)
    combine(NQ - 1)
    for q in range(NQ - 3, NQ):
        spread(q)
    for q in range(NQ - 3, NQ):
        finish(q)

    with jax.named_scope("end"):
        @pl.when(source)
        def _():
            all_bytes(lsend.at[pl.ds(0, NT - 1)], l_ss)
        all_bytes(lrecv.at[pl.ds(0, NG - 1)], k_ss)
        all_bytes(qsend.at[pl.ds(0, NY - 1)], q_ss)
        all_bytes(t1send.at[pl.ds(0, NY - 1)], t1_ss)
        for n in range(NL // 2):
            all_bytes(t3send.at[pl.ds(0, NY - 1), :, pl.ds(16 * n, 16)], t3_ss.at[n])
        for n in range(14):
            all_bytes(fall.at[0], rs_ss.at[n])
        for pair in range(2):
            all_bytes(send1.at[pair, pl.ds(0, NT - 1)], s1_ss.at[pair])
            all_bytes(send2a.at[pair, pl.ds(0, NT - 1)], s2_ss.at[pair])
        for q, (l0, nl) in enumerate(CHUNKS):
            lats = pl.ds(l0, nl)
            if q > 0:
                all_bytes(send2b.at[pl.ds(l0 - 2, nl), pl.ds(0, NT - 1)], s2_ss.at[q + 1])
            all_bytes(hrecv.at[lats], h_ss.at[q])
            all_bytes(mrecv.at[lats, pl.ds(0, NX4 - 1)], m_ss.at[q])
            all_bytes(mrecv.at[lats, pl.ds(0, NX4 - 1)], a_ss.at[q])
            all_bytes(hrecv.at[lats], b_ss.at[q])


def write_out(o, m, v, new_h, mean_h, var_h, sem):
    pieces = [(o.at[b], new_h.at[b]) for b in range(NB)]
    for n in range(2):
        half = pl.ds(n * (NL // 2), NL // 2)
        pieces += [(m.at[half], mean_h.at[half]), (v.at[half], var_h.at[half])]
    copies = [pltpu.make_async_copy(s, d, sem.at[n]) for n, (s, d) in enumerate(pieces)]
    for c in copies:
        c.start()
    for c in copies:
        c.wait()


def per_device(grid_state, noise_field, legendre, diffusion, input_weight, noise_weight, input_bias,
               middle_weight, output_weight):
    hbm = pl.BlockSpec(memory_space=pltpu.HBM)
    vm = pl.BlockSpec(memory_space=pltpu.VMEM)
    dma = pltpu.SemaphoreType.DMA
    V = pltpu.VMEM
    shapes = (((NB, NL, NX, C), BF16), ((NL, NX, C), F32), ((NL, NX, C), F32))
    held = pl.pallas_call(
        kernel,
        out_shape=tuple(V(s, d) for s, d in shapes),
        in_specs=[hbm] * 9,
        out_specs=(vm, vm, vm),
        scratch_shapes=[
            V((NB, NL, NX, C), BF16), V((NB, NL, NX, C), BF16), V((NL, C, C), BF16), V((1, C), F32),
            V((H, H), BF16), V((1, H), F32), V((H, H), BF16), V((H, C), BF16),
            V((NT, NX), F32), V((NT, NX), F32), V((2 * C, NX), BF16), V((NX, 2 * C), BF16),
            V((NT, 4 * NL, C), BF16), V((NZ, NY, 4 * NL, C), BF16),
            V((NY, NL * NW, C), BF16), V((NY, NL * NW, C), BF16),
            V((2, NT, NL * 2 * J, C), BF16), V((2, NT, NL * 2 * J, C), BF16),
            V((2, NT, 4 * J, C), BF16), V((2, NT, 4 * J, C), BF16),
            V((NL - 2, NT, 4 * J, C), BF16), V((NL - 2, NT, 4 * J, C), BF16),
            V((NY, 2 * NB, NL * NW, C), BF16), V((NY, 2 * NB, NL * NW, C), BF16),
            V((NY, 2 * NB, NL * NW, C), BF16), V((NY, 2 * NB, NL * NW, C), BF16),
            V((NR, NY * NL * NW), BF16), V((NY * NL * NW, NR), BF16), V((NR, C), F32), V((2 * NB, NR, C), F32),
            V((7, NR, C), BF16), V((7, NR, C), BF16), V((NZ, NR, C), BF16),
            V((NT * NL * 2 * J, C), F32), V((NT * NL * 2 * J, C), F32),
            V((NL - 2, NT * 4 * J, C), F32), V((NT * 4 * J, C), F32),
            V((3, NT * NL, C), BF16), V((3, C, NT * NL), BF16), V((3, C, C), F32),
            V((NL, 2, NX4, 2, MX, C), BF16), V((NL, NX4, 2, MX, C), BF16),
            V((NL, NX4, 2, MX, C), BF16), V((NL, NX4, 2, MX, C), BF16),
            V((NL, 2, MX, C), BF16), V((NL, 2, NX4, 2, MX, C), BF16),
            dma((12,)), dma, dma, dma, dma, dma, dma, dma, dma, dma((NL // 2,)), dma((NL // 2,)),
            dma((14,)), dma((14,)),
            dma((2,)), dma((2,)), dma((NQ + 1,)), dma((NQ + 1,)),
            dma((NQ,)), dma((NQ,)), dma((NQ,)), dma((NQ,)), dma((NQ,)), dma((NQ,)), dma((NQ,)), dma((NQ,)),
        ],
        compiler_params=pltpu.CompilerParams(
            collective_id=0, has_side_effects=True, vmem_limit_bytes=48 * 1024 * 1024),
    )(*[pltpu.with_memory_space_constraint(a, pltpu.HBM) for a in (
        grid_state, noise_field, legendre, diffusion[None, :], input_weight, noise_weight, input_bias[None, :],
        middle_weight, output_weight)])
    return pl.pallas_call(
        write_out,
        out_shape=tuple(jax.ShapeDtypeStruct(s, d) for s, d in shapes),
        in_specs=[vm] * 3,
        out_specs=(hbm,) * 3,
        scratch_shapes=[dma((8,))],
        compiler_params=pltpu.CompilerParams(vmem_limit_bytes=1024 * 1024),
    )(*[pltpu.with_memory_space_constraint(a, pltpu.VMEM) for a in held])

def solution(mesh):
    in_specs = (P("grp", "lat", None, None), P("grp", "lat", None, None), P("lat", None, None)) + (P(),) * 6
    out_specs = (P("grp", "lat", None, None), P("lat", None, None), P("lat", None, None))
    return jax.shard_map(per_device, mesh=mesh, in_specs=in_specs, out_specs=out_specs, check_vma=False)
```

```python
import math

import jax
import jax.numpy as jnp
from jax import lax
from jax.experimental import pallas as pl
from jax.experimental.pallas import tpu as pltpu
from jax.sharding import PartitionSpec as P

MESH = pl.DeviceIdType.MESH
F32 = jnp.float32
BF16 = jnp.bfloat16

NY, NZ = 4, 8
NT = NY * NZ
NX4 = 4
NG = 8
NB = 4
NP = 2
NL = 6
NX = 384
C = 128
H = 256
MX = NX // NG
CHUNKS = ((0, 2), (2, 1), (3, 1), (4, 1), (5, 1))
NQ = len(CHUNKS)
MATES = ((2, 0), (2, 1), (1, 0), (3, 0), (1, 1), (3, 1), (0, 1))
LINE = (2, 1, 3)
J = 6
NW = 8
OFFS = (0, 32, 60, 84, 104, 120, 132, 140)
NR = 144


def dot(a, b):
    return jnp.dot(a, b, preferred_element_type=F32)


def silu(v):
    u = 0.5 * v
    return u + u * jnp.tanh(u)


def angle(lon, wave):
    return lax.rem(lon * wave, NX).astype(F32) * (2.0 * math.pi / NX)


def all_bytes(ref, sem):
    pltpu.make_async_copy(ref, ref, sem).wait()


def band_column(col):
    wave = jnp.zeros_like(col)
    start = jnp.zeros_like(col)
    for w in range(1, NW):
        wave = wave + jnp.where(col >= OFFS[w], 1, 0)
        start = start + jnp.where(col >= OFFS[w], OFFS[w] - OFFS[w - 1], 0)
    return wave, col - start + NY * wave


def kernel(
    grid_h, noise_h, leg_h, diff_h, win_h, wnoise_h, bias_h, wmid_h, wout_h,
    obuf, mbuf, vbuf,
    gbuf, nbuf, leg, diff, wcat, bias, wmid, wout, cosa, sina, tf, ti,
    lsend, lrecv, qsend, qrecv, send1, recv1, send2a, recv2a, send2b, recv2b,
    t1send, t1recv, t3send, t3recv, dmat, dtm, scale3, rf, rs_send, rs_recv, fall,
    zf, work_a, work_b, work_c, pn, pt, dm,
    msend, hrecv, csend, mrecv, asend, arecv,
    in_sem, l_ss, l_rs, k_ss, k_rs, q_ss, q_rs, t1_ss, t1_rs, t3_ss, t3_rs, rs_ss, rs_rs,
    s1_ss, s1_rs, s2_ss, s2_rs, h_ss, h_rs, m_ss, m_rs, a_ss, a_rs, b_ss, b_rs,
):
    lat, mg = lax.axis_index("lat"), lax.axis_index("grp")
    my, mz = lat // NZ, lax.rem(lat, NZ)
    me = mz * NY + my
    mx, mc = mg // 2, lax.rem(mg, 2)
    iota = lambda shape, dim: lax.broadcasted_iota(jnp.int32, shape, dim)

    def visit(j, dy, body):
        half = (j + 1) // 2
        dz = jnp.where(lax.rem(j, 2) == 1, NZ - half, half)
        y, z = lax.rem(my + dy, NY), lax.rem(mz + dz, NZ)
        body(y * NZ + z, z * NY + y)

    def each_peer(body):
        def step(n, carry):
            k = NT - n
            visit(k // NY, lax.rem(k, NY), body)
            return carry
        lax.fori_loop(1, NT, step, 0)

    def each_row(dy, body):
        def step(n, carry):
            visit(NZ - 1 - n, dy, body)
            return carry
        lax.fori_loop(0, NZ - (1 if dy == 0 else 0), step, 0)

    def each_mate(body):
        for dx, dc in MATES:
            body(lax.rem(mx + dx, NX4) * 2 + lax.rem(mc + dc, 2))

    def each_y(body):
        for dy in (2, 1, 3):
            y = lax.rem(my + dy, NY)
            body(y, y * NZ + mz)

    def around(d):
        return lax.rem(mz + d + NZ, NZ)

    def send(src, dst, ss, rs, lat_id):
        pltpu.make_async_remote_copy(
            src_ref=src, dst_ref=dst, send_sem=ss, recv_sem=rs,
            device_id={"lat": lat_id}, device_id_type=MESH).start()

    turn = 1 - 2 * mc

    def at(d):
        return my * NZ + around(turn * d)

    loads = [
        (grid_h.at[0], gbuf.at[0]), (grid_h.at[1], gbuf.at[1]), (grid_h.at[2], gbuf.at[2]), (grid_h.at[3], gbuf.at[3]),
        (leg_h, leg), (diff_h, diff), (win_h, wcat.at[pl.ds(0, C)]), (wnoise_h, wcat.at[pl.ds(C, C)]),
        (bias_h, bias), (wmid_h, wmid), (wout_h, wout), (noise_h, nbuf),
    ]
    loads = [pltpu.make_async_copy(s, d, in_sem.at[n]) for n, (s, d) in enumerate(loads)]
    loads[0].start()
    loads[1].start()
    barrier = pltpu.get_barrier_semaphore()
    each_peer(lambda t, s: pl.semaphore_signal(
        barrier, inc=1, device_id={"lat": t}, device_id_type=MESH))
    each_mate(lambda g: pl.semaphore_signal(
        barrier, inc=1, device_id={"grp": g}, device_id_type=MESH))
    for c in loads[2:]:
        c.start()

    with jax.named_scope("tables"):
        base = angle(iota((NT, NX), 1), iota((NT, NX), 0))
        cosa[...] = jnp.cos(base)
        sina[...] = jnp.sin(base)
        part = iota((8, NX), 0)
        step = angle(iota((8, NX), 1), NT * lax.rem(part, 4))
        scale = math.sqrt(2.0 / NX)
        cosb, sinb = scale * jnp.cos(step), scale * jnp.sin(step)
        real = part < 4
        u, v = jnp.where(real, cosb, -sinb), jnp.where(real, -sinb, -cosb)
        for j in range(J):
            k = 4 * (j // 3) + j % 3
            tf[pl.ds(NT * j, NT), :] = (cosa[...] * u[k:k + 1] + sina[...] * v[k:k + 1]).astype(BF16)
        row = iota((NT, NX), 0)
        high = angle(iota((NT, NX), 1), NY * lax.rem(row, NW) + row // NW)
        cosq, sinq = jnp.cos(high), jnp.sin(high)
        for q in range(NY):
            co, si = cosq[NW * q:NW * (q + 1)], sinq[NW * q:NW * (q + 1)]
            pair = [co * u[k:k + 1] + si * v[k:k + 1] for k in (3, 7)]
            tf[pl.ds(J * NT + 16 * q, 16), :] = jnp.concatenate(pair, axis=0).astype(BF16)

    def forward(b):
        loads[b].wait()
        for n in range(NL // 2):
            rhs = jnp.concatenate([gbuf[b, 2 * n], gbuf[b, 2 * n + 1]], axis=1)
            out = dot(tf[...], rhs)
            high = []
            for k in range(2):
                lanes = out[:, k * C:(k + 1) * C]
                for j in range(J):
                    zf[pl.ds((2 * n + k) * 2 * J + (b % 2) * J + j, NT, stride=NL * 2 * J), :] = (
                        lanes[NT * j:NT * (j + 1)])
                high.append(lanes[J * NT:].reshape(NY, 2, NW, C))
            high = jnp.concatenate(high, axis=2).astype(BF16)
            for r in range(2):
                t1send[:, r * NB + b, pl.ds(16 * n, 16), :] = high[:, r]

    def pack(pair):
        send1[pair] = zf[...].astype(BF16).reshape(NT, NL * 2 * J, C)
        recv1[pair, me] = send1[pair, me]

    def send_first(pair, dy):
        each_row(dy, lambda t, s: send(
            send1.at[pair, s], recv1.at[pair, me], s1_ss.at[pair], s1_rs.at[pair], t))

    with jax.named_scope("F"):
        forward(0)
        forward(1)
        pack(0)
        forward(2)
        forward(3)
        pack(1)
    loads[4].wait()
    source = mz == mg
    with jax.named_scope("basis"):
        work_a[pl.ds(0, NL * C), :] = leg[...].astype(F32).reshape(NL * C, C)
        for q in range(NY):
            band = [work_a[pl.ds(C * l + 3 * NT + q, NW, stride=NY), :] for l in range(NL)]
            qsend[q] = jnp.concatenate(band, axis=0).astype(BF16)

        @pl.when(source)
        def _():
            def pack_leg(p, carry):
                lsend[p] = work_a[pl.ds(p, 4 * NL, stride=NT), :].astype(BF16)
                return carry
            lax.fori_loop(0, NT, pack_leg, 0)

    with jax.named_scope("barrier"):
        pl.semaphore_wait(barrier, NT - 1 + NG - 1)

    send_first(0, 0)
    each_y(lambda y, t: send(qsend.at[y], qrecv.at[my], q_ss, q_rs, t))
    each_y(lambda y, t: send(t1send.at[y], t1recv.at[my], t1_ss, t1_rs, t))

    @pl.when(source)
    def _():
        each_peer(lambda t, s: send(lsend.at[s], lrecv.at[mz, my], l_ss, l_rs, t))
        lrecv[mz, my] = lsend[me]
    send_first(1, 0)
    send_first(0, 1)
    qrecv[my] = qsend[my]
    t1recv[my] = t1send[my]
    with jax.named_scope("prep"):
        loads[5].wait()
        rows = iota((C, C), 0)

        def damp_at(degree):
            ratio = degree.astype(F32) * (degree.astype(F32) + 1.0) / float((C - 1) * C)
            return 1.0 / (1.0 + diff[...] * (ratio * ratio))
        damp = damp_at(rows)
        for i in range(3):
            dm[i] = jnp.where(rows >= me + NT * i, damp, 0.0)
        wave, degree = band_column(iota((NR, C), 0))
        scale3[...] = jnp.where(degree >= NY * wave + my, damp_at(degree + 3 * NT), 0.0)
    with jax.named_scope("w_q"):
        all_bytes(qrecv.at[pl.ds(0, NY - 1)], q_rs)
    with jax.named_scope("dmat"):
        col = iota((C, 2 * C), 1)
        _, degree = band_column(col)
        pick = jnp.where((col < NR) & (iota((C, 2 * C), 0) == degree + 3 * NT), 1.0, 0.0).astype(BF16)
        spread = dot(qrecv[...].reshape(NY * NL * NW, C), pick)
        wave, _ = band_column(iota((NY * NL * NW, 2 * C), 1))
        spread = jnp.where(lax.rem(iota((NY * NL * NW, 2 * C), 0), NW) == wave, spread, 0.0)
        dtm[...] = spread[:, :NR].astype(BF16)
        dmat[...] = spread.T[:NR].astype(BF16)
    with jax.named_scope("w_t1"):
        all_bytes(t1recv.at[pl.ds(0, NY - 1)], t1_rs)
    with jax.named_scope("R"):
        for k in range(0, 8, 2):
            both = [t1recv[:, k + e].reshape(NY * NL * NW, C) for e in range(2)]
            out = dot(dmat[...], jnp.concatenate(both, axis=1))
            rf[k] = out[:, :C]
            rf[k + 1] = out[:, C:]

    def ring_send(n, src, dst, hop):
        send(src, dst, rs_ss.at[n], rs_rs.at[n], at(hop))

    def ring_wait(*ids):
        for n in ids:
            all_bytes(fall.at[0], rs_rs.at[n])

    first = ((4, 2), (3, 1), (-3, -1))
    for n, (dest, hop) in enumerate(first):
        rs_send[n] = rf[around(turn * dest)].astype(BF16)
    for n, (dest, hop) in enumerate(first):
        ring_send(n, rs_send.at[n], rs_recv.at[n], hop)
    send_first(0, 2)
    with jax.named_scope("prep2"):
        ti[...] = tf[...].astype(F32).T.astype(BF16)
    with jax.named_scope("w_rsA"):
        ring_wait(0, 1, 2)
    rs_send[3] = (rf[around(turn * 2)] + rs_recv[0].astype(F32) + rs_recv[1].astype(F32)).astype(BF16)
    rs_send[4] = (rf[around(turn * -2)] + rs_recv[2].astype(F32)).astype(BF16)
    ring_send(3, rs_send.at[3], rs_recv.at[3], 1)
    ring_send(4, rs_send.at[4], rs_recv.at[4], -1)
    send_first(0, 3)
    send_first(1, 1)
    with jax.named_scope("w_rsB"):
        ring_wait(3, 4)
    rs_send[5] = (rf[around(turn)] + rs_recv[3].astype(F32)).astype(BF16)
    rs_send[6] = (rf[around(-turn)] + rs_recv[4].astype(F32)).astype(BF16)
    ring_send(5, rs_send.at[5], rs_recv.at[5], 1)
    ring_send(6, rs_send.at[6], rs_recv.at[6], -1)
    send_first(1, 2)
    with jax.named_scope("w_leg"):
        @pl.when(source)
        def _():
            all_bytes(lrecv.at[mg, pl.ds(0, NY - 1)], l_rs)

        @pl.when(jnp.logical_not(source))
        def _():
            all_bytes(lrecv.at[mg], l_rs)
    each_mate(lambda g: pltpu.make_async_remote_copy(
        src_ref=lrecv.at[mg], dst_ref=lrecv.at[mg],
        send_sem=k_ss, recv_sem=k_rs, device_id={"grp": g}, device_id_type=MESH).start())
    with jax.named_scope("w_rsC"):
        ring_wait(5, 6)
    total = rf[mz] + rs_recv[5].astype(F32) + rs_recv[6].astype(F32)
    fall[mz] = (total * scale3[...]).astype(BF16)
    ring_send(7, fall.at[mz], fall.at[mz], 1)
    ring_send(8, fall.at[mz], fall.at[mz], -1)
    send_first(1, 3)
    with jax.named_scope("w_k"):
        all_bytes(lrecv.at[pl.ds(0, NG - 1)], k_rs)
    with jax.named_scope("prepP"):
        work_a[pl.ds(0, NT * 4 * NL), :] = lrecv[...].astype(F32).reshape(NT * 4 * NL, C)
        for i in range(3):
            basis = jnp.concatenate(
                [work_a[pl.ds(4 * l + i, NT, stride=4 * NL), :] for l in range(NL)], axis=0)
            pn[i] = basis.astype(BF16)
            pt[i] = basis.T.astype(BF16)

    def analyse(pair):
        with jax.named_scope("w_a1"):
            all_bytes(recv1.at[pair, pl.ds(0, NT - 1)], s1_rs.at[pair])

        def member(k, carry):
            for i in range(3):
                halves = [jnp.concatenate(
                    [work_a[pl.ds(2 * J * l + J * k + 3 * r + i, NT, stride=NL * 2 * J), :] for l in range(NL)],
                    axis=0).astype(BF16) for r in range(2)]
                spec = dot(pt[i], jnp.concatenate(halves, axis=1))
                scale = dm[i]
                filt = (spec * jnp.concatenate([scale, scale], axis=1)).astype(BF16)
                back = dot(pn[i], filt)
                for r in range(2):
                    j = 3 * r + i
                    for l in range(NL):
                        rows = back[NT * l:NT * (l + 1), r * C:(r + 1) * C]
                        if l < 2:
                            work_c[pl.ds(2 * J * l + J * k + j, NT, stride=4 * J), :] = rows
                        else:
                            work_b[l - 2, pl.ds(2 * J * pair + J * k + j, NT, stride=4 * J), :] = rows
            return carry
        with jax.named_scope("S"):
            work_a[...] = recv1[pair].astype(F32).reshape(NT * NL * 2 * J, C)
            lax.fori_loop(0, 2, member, 0)
            send2a[pair] = work_c[...].astype(BF16).reshape(NT, 4 * J, C)
            if pair == 1:
                for l in range(NL - 2):
                    send2b[l] = work_b[l].astype(BF16).reshape(NT, 4 * J, C)
        each_peer(lambda t, s: send(send2a.at[pair, s], recv2a.at[pair, me], s2_ss.at[pair], s2_rs.at[pair], t))
        recv2a[pair, me] = send2a[pair, me]

    with jax.named_scope("w_agA"):
        ring_wait(7, 8)
    for n, side in ((9, -1), (10, 1)):
        near = around(turn * side)
        ring_send(n, fall.at[near], fall.at[near], -side)
    analyse(0)
    with jax.named_scope("w_agB"):
        ring_wait(9, 10)
    for n, side, hop in ((12, -2, 2), (11, -2, 1), (13, 2, -1)):
        far = around(turn * side)
        ring_send(n, fall.at[far], fall.at[far], hop)
    analyse(1)
    with jax.named_scope("w_agC"):
        ring_wait(11, 12, 13)
    with jax.named_scope("synth"):
        for k in range(0, 8, 2):
            out = dot(dtm[...], jnp.concatenate([fall[k], fall[k + 1]], axis=1)).astype(BF16)
            t3send[:, k] = out[:, :C].reshape(NY, NL * NW, C)
            t3send[:, k + 1] = out[:, C:].reshape(NY, NL * NW, C)
    for n in range(NL // 2):
        rows = pl.ds(16 * n, 16)
        each_y(lambda y, t: send(
            t3send.at[y, :, rows], t3recv.at[my, :, rows], t3_ss.at[n], t3_rs.at[n], t))
    with jax.named_scope("s2b"):
        for q in range(1, NQ):
            l0, nl = CHUNKS[q]
            lats = pl.ds(l0 - 2, nl)
            each_peer(lambda t, s: send(
                send2b.at[lats, s], recv2b.at[lats, me], s2_ss.at[q + 1], s2_rs.at[q + 1], t))
    t3recv[my] = t3send[my]
    for l in range(NL - 2):
        recv2b[l, me] = send2b[l, me]

    def join(q):
        l0, nl = CHUNKS[q]
        lats = pl.ds(l0, nl)
        with jax.named_scope("w_h"):
            all_bytes(hrecv.at[lats], h_rs.at[q])

        def one(x, carry):
            mine, theirs = msend[lats, mc, x, 0].astype(F32), hrecv[lats, x, 0].astype(F32)
            off = mine - theirs
            square = msend[lats, mc, x, 1].astype(F32) + hrecv[lats, x, 1].astype(F32)
            csend[lats, x, 0] = (mine + theirs).astype(BF16)
            csend[lats, x, 1] = (square + off * off * (1.0 / (2 * NB))).astype(BF16)
            return carry
        lax.fori_loop(0, NX4, one, 0)
        for dx in LINE:
            x = lax.rem(mx + dx, NX4)
            pltpu.make_async_remote_copy(
                src_ref=csend.at[lats, x], dst_ref=mrecv.at[lats, mx],
                send_sem=m_ss.at[q], recv_sem=m_rs.at[q],
                device_id={"grp": x * 2 + mc}, device_id_type=MESH).start()
        mrecv[lats, mx] = csend[lats, mx]

    def combine(q):
        l0, nl = CHUNKS[q]
        with jax.named_scope("w_m"):
            all_bytes(mrecv.at[pl.ds(l0, nl), pl.ds(0, NX4 - 1)], m_rs.at[q])
        lats = pl.ds(l0, nl)
        total = mrecv[lats, 0, 0].astype(F32)
        square = mrecv[lats, 0, 1].astype(F32)
        for x in range(1, NX4):
            total += mrecv[lats, x, 0].astype(F32)
            square += mrecv[lats, x, 1].astype(F32)
        mean = total * (1.0 / (NB * NG))
        for x in range(NX4):
            off = mrecv[lats, x, 0].astype(F32) * (1.0 / (2 * NB)) - mean
            square += (2 * NB) * (off * off)
        asend[lats, 0] = mean.astype(BF16)
        asend[lats, 1] = (square * (1.0 / (NB * NG - 1))).astype(BF16)
        for dx in LINE:
            pltpu.make_async_remote_copy(
                src_ref=asend.at[lats], dst_ref=arecv.at[lats, mc, mx],
                send_sem=a_ss.at[q], recv_sem=a_rs.at[q],
                device_id={"grp": lax.rem(mx + dx, NX4) * 2 + mc}, device_id_type=MESH).start()
        arecv[lats, mc, mx] = asend[lats]

    def spread(q):
        l0, nl = CHUNKS[q]
        lats = pl.ds(l0, nl)
        with jax.named_scope("w_ag"):
            all_bytes(mrecv.at[lats, pl.ds(0, NX4 - 1)], a_rs.at[q])
        pltpu.make_async_remote_copy(
            src_ref=arecv.at[lats, mc], dst_ref=arecv.at[lats, mc],
            send_sem=b_ss.at[q], recv_sem=b_rs.at[q],
            device_id={"grp": mx * 2 + 1 - mc}, device_id_type=MESH).start()

    def finish(q):
        l0, nl = CHUNKS[q]
        lats = pl.ds(l0, nl)
        with jax.named_scope("w_b"):
            all_bytes(hrecv.at[lats], b_rs.at[q])
        for g in range(NG):
            mbuf[lats, pl.ds(MX * g, MX), :] = arecv[lats, g % 2, g // 2, 0].astype(F32)
            vbuf[lats, pl.ds(MX * g, MX), :] = arecv[lats, g % 2, g // 2, 1].astype(F32)

    for c in loads[6:]:
        c.wait()
    for q, (l0, nl) in enumerate(CHUNKS):
        if l0 % 2 == 0:
            with jax.named_scope("w_t3"):
                all_bytes(t3recv.at[pl.ds(0, NY - 1), :, pl.ds(8 * l0, 16)], t3_rs.at[l0 // 2])
        with jax.named_scope("w_a2"):
            if q == 0:
                for pair in range(2):
                    all_bytes(recv2a.at[pair, pl.ds(0, NT - 1)], s2_rs.at[pair])
            else:
                all_bytes(recv2b.at[pl.ds(l0 - 2, nl), pl.ds(0, NT - 1)], s2_rs.at[q + 1])

        def column(l, pair):
            area = work_a.at[pl.ds(pair * NT * 4 * J, NT * 4 * J)]
            if l < 2:
                area[...] = recv2a[pair].astype(F32).reshape(NT * 4 * J, C)
                first = 2 * J * l
            else:
                area[...] = recv2b[l - 2].astype(F32).reshape(NT * 4 * J, C)
                first = 2 * J * pair
            sides = []
            for k in range(2):
                rows = [area[pl.ds(first + J * k + j, NT, stride=4 * J), :] for j in range(J)]
                for y in range(NY):
                    for r in range(2):
                        two = t3recv[y, r * NB + 2 * pair + k, pl.ds(16 * (l // 2), 16), :].astype(F32)
                        rows.append(two[8 * (l % 2):8 * (l % 2) + 8])
                sides.append(jnp.concatenate(rows, axis=0).astype(BF16))
            smooth = dot(ti[...], jnp.concatenate(sides, axis=1))
            smooth = jnp.concatenate([smooth[:, :C], smooth[:, C:]], axis=0)
            noise = nbuf[pl.ds(2 * pair, 2), l].reshape(2 * NX, C)
            pre = dot(jnp.concatenate([smooth.astype(BF16), noise], axis=1), wcat[...])
            one = silu(pre + bias[...]).astype(BF16)
            two = silu(dot(one, wmid[...])).astype(BF16)
            new = (smooth + dot(two, wout[...])).astype(BF16)
            obuf[pl.ds(2 * pair, 2), l] = new.reshape(2, NX, C)
        with jax.named_scope("G"):
            for l in range(l0, l0 + nl):
                for pair in range(2):
                    column(l, pair)

        def moments(g, carry):
            lats = pl.ds(l0, nl)
            vals = [obuf[b, lats, pl.ds(MX * g, MX), :].astype(F32) for b in range(NB)]
            total = (vals[0] + vals[1]) + (vals[2] + vals[3])
            mean = total * (1.0 / NB)
            offs = [v - mean for v in vals]
            square = (offs[0] * offs[0] + offs[1] * offs[1]) + (offs[2] * offs[2] + offs[3] * offs[3])
            x, c = g // 2, lax.rem(g, 2)
            msend[lats, c, x, 0] = total.astype(BF16)
            msend[lats, c, x, 1] = square.astype(BF16)
            return carry
        with jax.named_scope("mom"):
            lax.fori_loop(0, NG, moments, 0)
        lats = pl.ds(l0, nl)
        pltpu.make_async_remote_copy(
            src_ref=msend.at[lats, 1 - mc], dst_ref=hrecv.at[lats],
            send_sem=h_ss.at[q], recv_sem=h_rs.at[q],
            device_id={"grp": mx * 2 + 1 - mc}, device_id_type=MESH).start()
        if 1 <= q < NQ - 1:
            join(q - 1)
        if 2 <= q < NQ - 1:
            combine(q - 2)
        if q >= NQ - 2:
            join(q)
    combine(NQ - 3)
    for q in range(NQ - 3):
        spread(q)
    for q in range(NQ - 3):
        finish(q)
    combine(NQ - 2)
    combine(NQ - 1)
    for q in range(NQ - 3, NQ):
        spread(q)
    for q in range(NQ - 3, NQ):
        finish(q)

    with jax.named_scope("end"):
        @pl.when(source)
        def _():
            all_bytes(lsend.at[pl.ds(0, NT - 1)], l_ss)
        all_bytes(lrecv.at[pl.ds(0, NG - 1)], k_ss)
        all_bytes(qsend.at[pl.ds(0, NY - 1)], q_ss)
        all_bytes(t1send.at[pl.ds(0, NY - 1)], t1_ss)
        for n in range(NL // 2):
            all_bytes(t3send.at[pl.ds(0, NY - 1), :, pl.ds(16 * n, 16)], t3_ss.at[n])
        for n in range(14):
            all_bytes(fall.at[0], rs_ss.at[n])
        for pair in range(2):
            all_bytes(send1.at[pair, pl.ds(0, NT - 1)], s1_ss.at[pair])
            all_bytes(send2a.at[pair, pl.ds(0, NT - 1)], s2_ss.at[pair])
        for q, (l0, nl) in enumerate(CHUNKS):
            lats = pl.ds(l0, nl)
            if q > 0:
                all_bytes(send2b.at[pl.ds(l0 - 2, nl), pl.ds(0, NT - 1)], s2_ss.at[q + 1])
            all_bytes(hrecv.at[lats], h_ss.at[q])
            all_bytes(mrecv.at[lats, pl.ds(0, NX4 - 1)], m_ss.at[q])
            all_bytes(mrecv.at[lats, pl.ds(0, NX4 - 1)], a_ss.at[q])
            all_bytes(hrecv.at[lats], b_ss.at[q])


def write_out(o, m, v, new_h, mean_h, var_h, sem):
    pieces = [(o.at[b], new_h.at[b]) for b in range(NB)]
    for n in range(2):
        half = pl.ds(n * (NL // 2), NL // 2)
        pieces += [(m.at[half], mean_h.at[half]), (v.at[half], var_h.at[half])]
    copies = [pltpu.make_async_copy(s, d, sem.at[n]) for n, (s, d) in enumerate(pieces)]
    for c in copies:
        c.start()
    for c in copies:
        c.wait()


def per_device(grid_state, noise_field, legendre, diffusion, input_weight, noise_weight, input_bias,
               middle_weight, output_weight):
    hbm = pl.BlockSpec(memory_space=pltpu.HBM)
    vm = pl.BlockSpec(memory_space=pltpu.VMEM)
    dma = pltpu.SemaphoreType.DMA
    V = pltpu.VMEM
    shapes = (((NB, NL, NX, C), BF16), ((NL, NX, C), F32), ((NL, NX, C), F32))
    held = pl.pallas_call(
        kernel,
        out_shape=tuple(V(s, d) for s, d in shapes),
        in_specs=[hbm] * 9,
        out_specs=(vm, vm, vm),
        scratch_shapes=[
            V((NB, NL, NX, C), BF16), V((NB, NL, NX, C), BF16), V((NL, C, C), BF16), V((1, C), F32),
            V((H, H), BF16), V((1, H), F32), V((H, H), BF16), V((H, C), BF16),
            V((NT, NX), F32), V((NT, NX), F32), V((2 * C, NX), BF16), V((NX, 2 * C), BF16),
            V((NT, 4 * NL, C), BF16), V((NZ, NY, 4 * NL, C), BF16),
            V((NY, NL * NW, C), BF16), V((NY, NL * NW, C), BF16),
            V((2, NT, NL * 2 * J, C), BF16), V((2, NT, NL * 2 * J, C), BF16),
            V((2, NT, 4 * J, C), BF16), V((2, NT, 4 * J, C), BF16),
            V((NL - 2, NT, 4 * J, C), BF16), V((NL - 2, NT, 4 * J, C), BF16),
            V((NY, 2 * NB, NL * NW, C), BF16), V((NY, 2 * NB, NL * NW, C), BF16),
            V((NY, 2 * NB, NL * NW, C), BF16), V((NY, 2 * NB, NL * NW, C), BF16),
            V((NR, NY * NL * NW), BF16), V((NY * NL * NW, NR), BF16), V((NR, C), F32), V((2 * NB, NR, C), F32),
            V((7, NR, C), BF16), V((7, NR, C), BF16), V((NZ, NR, C), BF16),
            V((NT * NL * 2 * J, C), F32), V((NT * NL * 2 * J, C), F32),
            V((NL - 2, NT * 4 * J, C), F32), V((NT * 4 * J, C), F32),
            V((3, NT * NL, C), BF16), V((3, C, NT * NL), BF16), V((3, C, C), F32),
            V((NL, 2, NX4, 2, MX, C), BF16), V((NL, NX4, 2, MX, C), BF16),
            V((NL, NX4, 2, MX, C), BF16), V((NL, NX4, 2, MX, C), BF16),
            V((NL, 2, MX, C), BF16), V((NL, 2, NX4, 2, MX, C), BF16),
            dma((12,)), dma, dma, dma, dma, dma, dma, dma, dma, dma((NL // 2,)), dma((NL // 2,)),
            dma((14,)), dma((14,)),
            dma((2,)), dma((2,)), dma((NQ + 1,)), dma((NQ + 1,)),
            dma((NQ,)), dma((NQ,)), dma((NQ,)), dma((NQ,)), dma((NQ,)), dma((NQ,)), dma((NQ,)), dma((NQ,)),
        ],
        compiler_params=pltpu.CompilerParams(
            collective_id=0, has_side_effects=True, vmem_limit_bytes=48 * 1024 * 1024),
    )(*[pltpu.with_memory_space_constraint(a, pltpu.HBM) for a in (
        grid_state, noise_field, legendre, diffusion[None, :], input_weight, noise_weight, input_bias[None, :],
        middle_weight, output_weight)])
    return pl.pallas_call(
        write_out,
        out_shape=tuple(jax.ShapeDtypeStruct(s, d) for s, d in shapes),
        in_specs=[vm] * 3,
        out_specs=(hbm,) * 3,
        scratch_shapes=[dma((8,))],
        compiler_params=pltpu.CompilerParams(vmem_limit_bytes=1024 * 1024),
    )(*[pltpu.with_memory_space_constraint(a, pltpu.VMEM) for a in held])

def solution(mesh):
    in_specs = (P("grp", "lat", None, None), P("grp", "lat", None, None), P("lat", None, None)) + (P(),) * 6
    out_specs = (P("grp", "lat", None, None), P("lat", None, None), P("lat", None, None))
    return jax.shard_map(per_device, mesh=mesh, in_specs=in_specs, out_specs=out_specs, check_vma=False)
```
